32 devices in a mesh: emb: 8 (over z, x), seq: 4 (over y, core).
Axes of the slice: x: 2, y: 2, z: 4, core: 2. Of those that a mesh axis runs over, the one named last changes fastest.
Arguments:
- item_table: bfloat16 [32768, 512], P('emb'), may hold values from -6 to 6
- fetch_rows: int32 [8, 4, 8, 64], P('emb', 'seq'), may hold values from 0 to 4095
- event_slot: int32 [32768], P(('emb', 'seq')), may hold values from 0 to 511, as said below
- lengths: int32 [32, 8], P(('emb', 'seq')), may hold values from 1 to 512, 1024 in all within a row
- in_weight: bfloat16 [512, 2048], replicated, may hold values from -0.25 to 0.25
- out_weight: bfloat16 [512, 512], replicated, may hold values from -0.25 to 0.25
- out_grad: bfloat16 [32768, 512], P(('emb', 'seq')), may hold values from -6 to 6
Outputs:
- layer_out: bfloat16 [32768, 512], P(('emb', 'seq'))
- table_grad: float32 [32768, 512], P(('emb', 'seq'))
- in_weight_grad: float32 [512, 2048], replicated
- out_weight_grad: float32 [512, 512], replicated
The draws below stay inside these ranges and needn't reach their ends.
Inputs may be any that keep to these rules, and one draw needn't show every extreme that they name: `event_slot`: within each buffer of 1024 events every slot 0 to 511 is named by at least one event.
All inputs are finite; a program needn't handle non-finite values.
Results may differ from the reference program's by a relative error of at most 0.02.
Values may be sent and summed in bfloat16 or wider, within the bound.
No kernel may reach another device: no remote copies, remote signals or barrier semaphores. Data moves between devices by JAX's collectives and lax.ppermute only.
A program may use at most 192 MiB of HBM per device.

```python
import math
import jax
import jax.numpy as jnp
import numpy as np
from jax import lax

D = 512
HEADS = 4
TOK_DEV = 1024
SEQ_DEV = 8
MOST = 512
SLOTS = 512
CAP = 64
R_SHARD = 4096
ROWS = 32768
BUFFERS = 32
TOKENS = 32768
N_EMB = 8
N_SEQ = 4


def draw_event_slot(key, part):
    buffer_keys = jax.random.split(jax.random.fold_in(key, 17), BUFFERS)

    def one_buffer(buffer_key):
        first_key, second_key, third_key = jax.random.split(buffer_key, 3)
        covered = jax.random.permutation(first_key, SLOTS).astype(jnp.int32)
        repeats = jax.random.randint(second_key, (TOK_DEV - SLOTS,), 0, SLOTS).astype(jnp.int32)
        joined = jnp.concatenate([covered, repeats])
        return jax.random.permutation(third_key, joined).astype(jnp.int32)
    return jax.vmap(one_buffer)(buffer_keys).reshape(TOKENS).astype(jnp.int32)


def with_ends(array, rng, least, largest):
    extent = array.shape
    place = [jax.random.randint(jax.random.fold_in(rng, axis), (), 0, extent[axis]) for axis in range(len(extent))]
    array = array.at[tuple(place)].set(least)
    longest = extent.index(max(extent))
    place[longest] = (place[longest] + 1) % extent[longest]
    return array.at[tuple(place)].set(largest)


def levels(own_key, dims, cuts, low, high):
    def one(position, shards_of):
        draws = jax.random.uniform(jax.random.fold_in(jax.random.fold_in(own_key, 6), position), (shards_of,), jnp.float32, low / len(cuts), high / len(cuts))
        return jnp.repeat(jnp.exp(draws), dims[position] // shards_of).reshape((-1,) + (1,) * (len(dims) - position - 1))

    level = one(*cuts[0])
    for cut in cuts[1:]:
        level = level * one(*cut)
    return level


def length_profile(amount, total, limit, lean):
    weights = [(1 << 20) // math.isqrt(grade ** lean) + 1 for grade in range(2, amount + 1)]
    rest, given = total - limit - (amount - 1), [1] * (amount - 1)
    while rest > 0:
        free = [i for i in range(amount - 1) if given[i] < limit]
        pool, left = sum([weights[i] for i in free]), rest
        for i in free:
            addition = min(limit - given[i], max(1, left * weights[i] // pool), rest)
            given[i] = given[i] + addition
            rest = rest - addition
    return np.array([limit] + given)


def ragged_sizes(own_key, number_of, total, most, slope):
    if number_of == 2:
        one = jax.random.randint(own_key, (), max(1, total - most), min(most, total - 1) + 1)
        return jnp.stack([one, total - one])
    sizes = jnp.asarray(length_profile(number_of, total, most, slope), jnp.int32)
    couples = (number_of - 1) // 2
    source_of, taker = sizes[1:1 + 2 * couples:2], sizes[2:2 + 2 * couples:2]
    margin = jnp.minimum(source_of - 1, most - taker)
    moved = jax.random.randint(jax.random.fold_in(own_key, 1), (couples,), 0, 1 << 20) % (margin + 1)
    sizes = sizes.at[1:1 + 2 * couples:2].set(source_of - moved).at[2:2 + 2 * couples:2].set(taker + moved)
    return sizes[jax.random.permutation(jax.random.fold_in(own_key, 2), number_of)]


def bell_draw(key, shape, scale, bound, cuts=(), kind=jnp.bfloat16):
    drawn = jax.random.normal(key, shape, jnp.float32) * scale
    if len(cuts) > 0:
        drawn = levels(key, shape, cuts, -0.22, 0.18) * drawn
    return jnp.clip(drawn, min=-bound, max=bound).astype(kind)


def setup_inputs(seed: int = 0) -> dict:
    splits = jax.random.split(jax.random.key(seed), 8)
    item_table = bell_draw(splits[0], (ROWS, D), 1.0, 6.0, ((0, 8),))
    fetch_rows = with_ends(jax.random.randint(splits[1], (N_EMB, N_SEQ, N_EMB, CAP), 0, R_SHARD), jax.random.fold_in(splits[1], 1), 0, R_SHARD - 1).astype(jnp.int32)
    event_slot = draw_event_slot(jax.random.fold_in(splits[7], 71), 0)
    lengths = jax.vmap(lambda own: ragged_sizes(own, SEQ_DEV, TOK_DEV, MOST, 2))(jax.random.split(splits[3], BUFFERS)).reshape((BUFFERS, SEQ_DEV)).astype(jnp.int32)
    in_weight = bell_draw(splits[4], (D, 4 * D), D ** -0.5, 0.25)
    out_weight = bell_draw(splits[5], (D, D), D ** -0.5, 0.25)
    out_grad = bell_draw(splits[6], (TOKENS, D), 1.0, 6.0, ((0, 32),))
    return dict(item_table=item_table, fetch_rows=fetch_rows, event_slot=event_slot, lengths=lengths, in_weight=in_weight, out_weight=out_weight, out_grad=out_grad)


EPS = 1e-05

def normalize(rows_in):
    center = rows_in - lax.optimization_barrier(jnp.mean(rows_in, axis=-1, keepdims=True))
    spread = lax.optimization_barrier(jnp.mean(center * center, axis=-1, keepdims=True))
    return center * lax.rsqrt(spread + EPS)

def hstu_layer(events, in_weight, out_weight, lengths_row):
    rows_count, model_width = events.shape
    head_size = model_width // HEADS
    normed = normalize(events.astype(jnp.float32)).astype(jnp.bfloat16)
    hidden = jax.nn.silu(jnp.dot(normed, in_weight, preferred_element_type=jnp.float32))
    update_gate = hidden[:, :model_width]
    values = hidden[:, model_width:2 * model_width].astype(jnp.bfloat16).reshape(rows_count, HEADS, head_size)
    queries = hidden[:, 2 * model_width:3 * model_width].astype(jnp.bfloat16).reshape(rows_count, HEADS, head_size)
    key_rows = hidden[:, 3 * model_width:].astype(jnp.bfloat16).reshape(rows_count, HEADS, head_size)
    scores = jnp.einsum('ihd,jhd->hij', queries, key_rows, preferred_element_type=jnp.float32) * head_size ** (-0.5)
    places = jnp.arange(rows_count, dtype=jnp.int32)
    seq_ends = jnp.cumsum(lengths_row).astype(jnp.int32)
    segment = lax.optimization_barrier(jnp.sum((places[:, None] >= seq_ends[None, :]).astype(jnp.int32), axis=1))
    allowed = (segment[:, None] == segment[None, :]) & (places[None, :] <= places[:, None])
    weights = jnp.where(allowed[None], jax.nn.silu(scores) / MOST, 0.0).astype(jnp.bfloat16)
    attended = jnp.einsum('hij,jhd->ihd', weights, values, preferred_element_type=jnp.float32).reshape(rows_count, model_width)
    gated_rows = (normalize(attended) * update_gate).astype(jnp.bfloat16)
    return (jnp.dot(gated_rows, out_weight, preferred_element_type=jnp.float32) + events.astype(jnp.float32)).astype(jnp.bfloat16)

def reference(item_table, fetch_rows, event_slot, lengths, in_weight, out_weight, out_grad):
    owners = (jnp.arange(SLOTS, dtype=jnp.int32) // CAP * R_SHARD).astype(jnp.int32)
    slot_rows = (fetch_rows.reshape(BUFFERS, SLOTS) + owners[None, :]).astype(jnp.int32)
    event_rows = jnp.take_along_axis(slot_rows, event_slot.reshape(BUFFERS, TOK_DEV).astype(jnp.int32), axis=1).astype(jnp.int32)
    events = item_table[event_rows]

    def one_buffer(totals, pieces):
        rows_in, lengths_row, grad_row = pieces

        def forward(rows_x, first, second):
            return hstu_layer(rows_x, first, second, lengths_row)
        result, pullback = jax.vjp(forward, rows_in, in_weight, out_weight)
        row_grad, first_grad, second_grad = pullback(grad_row)
        totals = (totals[0] + first_grad.astype(jnp.float32), totals[1] + second_grad.astype(jnp.float32))
        return (totals, (result, row_grad))
    start = (jnp.zeros((D, 4 * D), jnp.float32), jnp.zeros((D, D), jnp.float32))
    totals, outputs = lax.scan(one_buffer, start, (events, lengths, out_grad.reshape(BUFFERS, TOK_DEV, D)))
    results, row_grads = outputs
    table_grad = jax.ops.segment_sum(row_grads.reshape(TOKENS, D).astype(jnp.float32), event_rows.reshape(TOKENS), num_segments=ROWS)
    return (results.reshape(TOKENS, D), table_grad, totals[0], totals[1])
```

```python
import functools

import jax
import jax.numpy as jnp
from jax import lax
from jax.experimental import pallas as pl
from jax.experimental.pallas import tpu as pltpu
from jax.sharding import PartitionSpec as P

HEADS = 4
MOST = 512
EPS = 1e-05
BLOCK = 256
VMEM = pl.BlockSpec(memory_space=pltpu.VMEM)
SMEM = pl.BlockSpec(memory_space=pltpu.SMEM)
BF = jnp.bfloat16
F32 = jnp.float32


def mm(a, b):
    return jnp.dot(a, b, preferred_element_type=F32)


def mm_t(a, b):
    return lax.dot_general(a, b, (((1,), (1,)), ((), ())), preferred_element_type=F32)


def tt_mm(a, b):
    return lax.dot_general(a, b, (((0,), (0,)), ((), ())), preferred_element_type=F32)


def center_rows(x):
    center = x - jnp.mean(x, axis=-1, keepdims=True)
    spread = jnp.mean(center * center, axis=-1, keepdims=True)
    inverse = lax.rsqrt(spread + EPS)
    return center * inverse, inverse


def center_back(grad, normed, inverse):
    along = jnp.mean(grad * normed, axis=-1, keepdims=True)
    return inverse * (grad - jnp.mean(grad, axis=-1, keepdims=True) - normed * along)


def history_ends(len_ref):
    ends, total = [], 0
    for k in range(len_ref.shape[1]):
        total = total + len_ref[0, k]
        ends.append(total)
    return ends


def history_start(ends, place):
    start = jnp.zeros_like(place)
    for end in ends:
        start = jnp.maximum(start, jnp.where(place >= end, end, 0))
    return start


def first_kernel(
    len_ref, slot_row, slot_col, rows_ref, win_ref, wout_ref, og_ref,
    out_ref, vqk_ref, datt_ref, dsil_ref, nt_ref, wg_ref, dn_ref, res_ref,
    hid, gate, ev, att, gated, dgate,
):
    slots, width = rows_ref.shape
    tokens = og_ref.shape[0]
    head = width // HEADS
    half_scale = 0.5 * head**-0.5
    normed, _ = center_rows(rows_ref[...].astype(F32))
    normed = normed.astype(BF)
    nt_ref[...] = normed.T
    for j in range(4):
        cols = slice(j * width, (j + 1) * width)
        pre = mm(normed, win_ref[:, cols])
        sig = 0.5 + 0.5 * jnp.tanh(0.5 * pre)
        act = pre * sig
        hid[:, cols] = act.astype(BF)
        dsil_ref[:, cols] = (sig + act * (1.0 - sig)).astype(BF)

    def spread(i, _):
        span = pl.ds(pl.multiple_of(i * BLOCK, BLOCK), BLOCK)
        lane = lax.broadcasted_iota(jnp.int32, (BLOCK, slots), 1)
        pick = jnp.where(slot_col[span, :] == lane, 1.0, 0.0).astype(BF)
        ev[span, :] = mm(pick, rows_ref[...]).astype(BF)
        gate[span, :] = mm(pick, hid[:, :width]).astype(BF)
        for j in range(3):
            vqk_ref[span, j * width : (j + 1) * width] = mm(
                pick, hid[:, (j + 1) * width : (j + 2) * width]
            ).astype(BF)
        return 0

    lax.fori_loop(0, tokens // BLOCK, spread, 0)
    ends = history_ends(len_ref)

    def rows_step(i, _):
        base = pl.multiple_of(i * BLOCK, BLOCK)
        span = pl.ds(base, BLOCK)
        start = history_start(ends, base + lax.broadcasted_iota(jnp.int32, (BLOCK, 1), 0))
        place = base + lax.broadcasted_iota(jnp.int32, (BLOCK, BLOCK), 0)
        att[...] = jnp.zeros_like(att)

        def keys_step(j, _):
            key_base = pl.multiple_of(j * BLOCK, BLOCK)
            keys = pl.ds(key_base, BLOCK)
            other = key_base + lax.broadcasted_iota(jnp.int32, (BLOCK, BLOCK), 1)
            allowed = (other >= start) & (other <= place)
            for h in range(HEADS):
                lo = h * head
                q = vqk_ref[span, width + lo : width + lo + head]
                k = vqk_ref[keys, 2 * width + lo : 2 * width + lo + head]
                v = vqk_ref[keys, lo : lo + head]
                u = mm_t(q, k) * half_scale
                w = jnp.where(allowed, u + u * jnp.tanh(u), 0.0).astype(BF)
                att[:, lo : lo + head] += mm(w, v)
            return 0

        lax.fori_loop(history_start(ends, base) // BLOCK, i + 1, keys_step, 0)
        normed_att, inverse = center_rows(att[...] * (1.0 / MOST))
        g = gate[span, :].astype(F32)
        gated_rows = (normed_att * g).astype(BF)
        gated[span, :] = gated_rows
        out_ref[span, :] = (mm(gated_rows, wout_ref[...]) + ev[span, :].astype(F32)).astype(BF)
        dgated = mm_t(og_ref[span, :], wout_ref[...])
        dgate[span, :] = (dgated * normed_att).astype(BF)
        datt = center_back(dgated * g, normed_att, inverse)
        datt_ref[span, :] = (datt * (1.0 / MOST)).astype(BF)
        return 0

    lax.fori_loop(0, tokens // BLOCK, rows_step, 0)
    wg_ref[:width, :] = tt_mm(gated[...], og_ref[...]).astype(BF)
    put = jnp.where(
        slot_row[...] == lax.broadcasted_iota(jnp.int32, (slots, tokens), 0), 1.0, 0.0
    ).astype(BF)
    dpre = (mm(put, dgate[...]) * dsil_ref[:, :width].astype(F32)).astype(BF)
    wg_ref[width:, :] = mm(nt_ref[...], dpre).astype(BF)
    dn_ref[...] = mm_t(dpre, win_ref[:, :width])
    res_ref[...] = mm(put, og_ref[...])


def second_kernel(
    len_ref, slot_row, rows_ref, vqk_ref, datt_ref, dsil_ref, win_ref, dn_ref, res_ref,
    dpre_ref, grad_ref, dvqk,
):
    slots, width = rows_ref.shape
    tokens = datt_ref.shape[0]
    head = width // HEADS
    half_scale = 0.5 * head**-0.5
    ends = history_ends(len_ref)
    dvqk[...] = jnp.zeros_like(dvqk)

    def rows_step(i, _):
        base = pl.multiple_of(i * BLOCK, BLOCK)
        span = pl.ds(base, BLOCK)
        start = history_start(ends, base + lax.broadcasted_iota(jnp.int32, (1, BLOCK), 1))
        place = base + lax.broadcasted_iota(jnp.int32, (BLOCK, BLOCK), 1)

        def keys_step(j, _):
            key_base = pl.multiple_of(j * BLOCK, BLOCK)
            keys = pl.ds(key_base, BLOCK)
            other = key_base + lax.broadcasted_iota(jnp.int32, (BLOCK, BLOCK), 0)
            allowed = (other >= start) & (other <= place)
            for h in range(HEADS):
                lo = h * head
                vs = slice(lo, lo + head)
                qs = slice(width + lo, width + lo + head)
                ks = slice(2 * width + lo, 2 * width + lo + head)
                q, k, v = vqk_ref[span, qs], vqk_ref[keys, ks], vqk_ref[keys, vs]
                da = datt_ref[span, vs]
                u = mm_t(k, q) * half_scale
                th = jnp.tanh(u)
                w = jnp.where(allowed, u + u * th, 0.0).astype(BF)
                slope = (half_scale + half_scale * th) * (1.0 + u - u * th)
                ds = jnp.where(allowed, mm_t(v, da) * slope, 0.0).astype(BF)
                dvqk[keys, vs] += mm(w, da)
                dvqk[keys, ks] += mm(ds, q)
                dvqk[span, qs] += tt_mm(ds, k)
            return 0

        lax.fori_loop(history_start(ends, base) // BLOCK, i + 1, keys_step, 0)
        return 0

    lax.fori_loop(0, tokens // BLOCK, rows_step, 0)
    put = jnp.where(
        slot_row[...] == lax.broadcasted_iota(jnp.int32, (slots, tokens), 0), 1.0, 0.0
    ).astype(BF)
    dn = dn_ref[...]
    for j in range(3):
        cols = slice(j * width, (j + 1) * width)
        later = slice((j + 1) * width, (j + 2) * width)
        dpre = (mm(put, dvqk[:, cols].astype(BF)) * dsil_ref[:, later].astype(F32)).astype(BF)
        dpre_ref[:, cols] = dpre
        dn = dn + mm_t(dpre, win_ref[:, later])
    normed, inverse = center_rows(rows_ref[...].astype(F32))
    grad_ref[...] = (center_back(dn, normed, inverse) + res_ref[...]).astype(BF)


def third_kernel(nt_ref, dpre_ref, wg_ref):
    wg_ref[...] = mm(nt_ref[...], dpre_ref[...]).astype(BF)


def table_kernel(count, *refs):
    places, rows, out = refs[:count], refs[count : 2 * count], refs[-1]
    height = min(BLOCK, out.shape[0])

    def step(i, _):
        base = pl.multiple_of(i * height, height)
        total = None
        for place, row in zip(places, rows):
            at = base + lax.broadcasted_iota(jnp.int32, (height, place.shape[1]), 0)
            put = jnp.where(place[...] == at, 1.0, 0.0).astype(BF)
            part = mm(put, row[...])
            total = part if total is None else total + part
        out[pl.ds(base, height), :] = total
        return 0

    lax.fori_loop(0, out.shape[0] // height, step, 0)


def call(kernel, outs, scratch, specs, flops):
    return pl.pallas_call(
        kernel,
        out_shape=[jax.ShapeDtypeStruct(s, d) for s, d in outs],
        in_specs=specs,
        out_specs=[VMEM] * len(outs),
        scratch_shapes=[pltpu.VMEM(s, d) for s, d in scratch],
        compiler_params=pltpu.CompilerParams(vmem_limit_bytes=56 * 2**20),
        cost_estimate=pl.CostEstimate(flops=flops, bytes_accessed=10**7, transcendentals=0),
    )


AXES = ("emb", "seq")


def swap(x, seq_count, total, partner):
    return lax.ppermute(x, AXES, [(d, partner(d)) for d in range(total)])


def reduce_plan(emb_count, seq_count):
    total = emb_count * seq_count
    seq_bits = seq_count.bit_length() - 1
    emb_bits = emb_count.bit_length() - 1
    me = lax.axis_index("emb") * seq_count + lax.axis_index("seq")
    bit = lambda d, b: (d >> b) & 1
    pair = lambda b: (lambda d: d ^ (1 << b), bit(me, b))
    plan = []
    first = 0 if seq_bits else None
    plan.append(pair(0))
    a, b = seq_bits, 1
    plan.append(
        (lambda d: d ^ (1 << a if bit(d, 0) == 0 else 1 << b), jnp.where(bit(me, 0) == 0, bit(me, a), bit(me, b)))
    )
    plan.append(
        (lambda d: d ^ (1 << b if bit(d, 0) == 0 else 1 << a), jnp.where(bit(me, 0) == 0, bit(me, b), bit(me, a)))
    )
    rest = [k for k in range(1, seq_bits + emb_bits) if k not in (a, b)]
    return plan, rest, me, total


def weight_sum(x, emb_count, seq_count):
    plan, rest, me, total = reduce_plan(emb_count, seq_count)
    columns = x.shape[1]
    for partner, place in plan:
        halves = x.reshape(2, x.shape[0] // 2, columns)
        keep = lax.dynamic_index_in_dim(halves, place, 0, keepdims=False)
        give = lax.dynamic_index_in_dim(halves, 1 - place, 0, keepdims=False)
        got = swap(give, seq_count, total, partner)
        x = (keep.astype(F32) + got.astype(F32)).astype(BF)
    count = 1 << len(rest)
    spread = lambda m: sum(((m >> i) & 1) << b for i, b in enumerate(rest))
    place = sum(((me >> b) & 1) << i for i, b in enumerate(rest))
    parts = x.reshape(count, x.shape[0] // count, columns)
    total_x = lax.dynamic_index_in_dim(parts, place, 0, keepdims=False).astype(F32)
    for m in range(1, count):
        give = lax.dynamic_index_in_dim(parts, place ^ m, 0, keepdims=False)
        total_x = total_x + swap(give, seq_count, total, lambda d: d ^ spread(m)).astype(F32)
    x = total_x.astype(BF)
    whole = jnp.zeros((count,) + x.shape, BF)
    whole = lax.dynamic_update_index_in_dim(whole, x, place, 0)
    for m in range(1, count):
        whole = lax.dynamic_update_index_in_dim(
            whole, swap(x, seq_count, total, lambda d: d ^ spread(m)), place ^ m, 0
        )
    x = whole.reshape(-1, columns)
    for partner, place in plan[::-1]:
        got = swap(x, seq_count, total, partner)
        whole = jnp.zeros((2,) + x.shape, BF)
        whole = lax.dynamic_update_index_in_dim(whole, x, place, 0)
        whole = lax.dynamic_update_index_in_dim(whole, got, 1 - place, 0)
        x = whole.reshape(-1, columns)
    return x.astype(F32)


def on_device(item_table, fetch_rows, event_slot, lengths, in_weight, out_weight, out_grad):
    emb_count = lax.axis_size("emb")
    seq_count = lax.axis_size("seq")
    shard_rows, width = item_table.shape
    requests = fetch_rows.reshape(emb_count, -1)
    slots = requests.shape[0] * requests.shape[1]
    tokens = event_slot.shape[0]
    asked = lax.all_to_all(requests, "emb", split_axis=0, concat_axis=0, tiled=True)
    found = item_table[asked]
    fetched = lax.all_to_all(found, "emb", split_axis=0, concat_axis=0, tiled=True)
    rows = fetched.reshape(slots, width)
    slot_row, slot_col = event_slot.reshape(1, tokens), event_slot.reshape(tokens, 1)

    layer_out, vqk, datt, dsil, nt, wg1, dn, res = call(
        first_kernel,
        [
            ((tokens, width), BF), ((tokens, 3 * width), BF), ((tokens, width), BF), ((slots, 4 * width), BF),
            ((width, slots), BF), ((2 * width, width), BF), ((slots, width), F32), ((slots, width), F32),
        ],
        [
            ((slots, 4 * width), BF), ((tokens, width), BF), ((tokens, width), BF), ((BLOCK, width), F32),
            ((tokens, width), BF), ((tokens, width), BF),
        ],
        [SMEM] + [VMEM] * 6,
        10**10,
    )(lengths, slot_row, slot_col, rows, in_weight, out_weight, out_grad)
    wg1 = weight_sum(wg1, emb_count, seq_count)

    dpre, slot_grad = call(
        second_kernel,
        [((slots, 3 * width), BF), ((slots, width), BF)],
        [((tokens, 3 * width), F32)],
        [SMEM] + [VMEM] * 8,
        10**10,
    )(lengths, slot_row, rows, vqk, datt, dsil, in_weight, dn, res)
    (wg2,) = call(third_kernel, [((width, 3 * width), BF)], [], [VMEM] * 2, 10**9)(nt, dpre)
    wg2 = weight_sum(wg2, emb_count, seq_count)

    returned = lax.all_to_all(
        slot_grad.reshape(emb_count, -1, width), "emb", split_axis=0, concat_axis=0, tiled=True
    )
    arrays, places = [returned.reshape(slots, width)], [asked.reshape(1, slots)]
    for b in reversed(range(seq_count.bit_length() - 1)):
        other = [(s, s ^ (1 << b)) for s in range(seq_count)]
        places += [lax.ppermute(p, "seq", other) for p in places]
        arrays += [lax.ppermute(a, "seq", other) for a in arrays]
    quarter = shard_rows // seq_count
    base = lax.axis_index("seq") * quarter
    places = [p - base for p in places]
    (table_grad,) = call(
        functools.partial(table_kernel, len(places)),
        [((quarter, width), F32)],
        [],
        [VMEM] * (2 * len(places)),
        10**9,
    )(*places, *arrays)
    in_total = jnp.concatenate([wg1[width:], wg2], axis=1)
    return layer_out, table_grad, in_total, wg1[:width]


def solution(mesh):
    placed = (
        P("emb", None),
        P("emb", "seq", None, None),
        P(("emb", "seq")),
        P(("emb", "seq"), None),
        P(),
        P(),
        P(("emb", "seq"), None),
    )
    return jax.shard_map(
        on_device,
        mesh=mesh,
        in_specs=placed,
        out_specs=(P(("emb", "seq"), None), P(("emb", "seq"), None), P(), P()),
        check_vma=False,
    )
```

```python
import functools

import jax
import jax.numpy as jnp
from jax import lax
from jax.experimental import pallas as pl
from jax.experimental.pallas import tpu as pltpu
from jax.sharding import PartitionSpec as P


HEADS = 4
MOST = 512
EPS = 1e-05
BLOCK = 256
GROUPS = ((0, 2), (2, 3), (3, 4))
VMEM = pl.BlockSpec(memory_space=pltpu.VMEM)
SMEM = pl.BlockSpec(memory_space=pltpu.SMEM)
BF = jnp.bfloat16
F32 = jnp.float32


AXES = ("e1", "e0", "s1", "s0")


def mm(a, b):
    return jnp.dot(a, b, preferred_element_type=F32)


def mm_t(a, b):
    return lax.dot_general(a, b, (((1,), (1,)), ((), ())), preferred_element_type=F32)


def tt_mm(a, b):
    return lax.dot_general(a, b, (((0,), (0,)), ((), ())), preferred_element_type=F32)


def center_rows(x):
    center = x - jnp.mean(x, axis=-1, keepdims=True)
    spread = jnp.mean(center * center, axis=-1, keepdims=True)
    inverse = lax.rsqrt(spread + EPS)
    return center * inverse, inverse


def center_back(grad, normed, inverse):
    along = jnp.mean(grad * normed, axis=-1, keepdims=True)
    return inverse * (grad - jnp.mean(grad, axis=-1, keepdims=True) - normed * along)


def history_ends(len_ref):
    ends, total = [], 0
    for k in range(len_ref.shape[1]):
        total = total + len_ref[0, k]
        ends.append(total)
    return ends


def history_start(ends, place):
    start = jnp.zeros_like(place)
    for end in ends:
        start = jnp.maximum(start, jnp.where(place >= end, end, 0))
    return start


def one_hot_rows(slot_row, slots):
    at = lax.broadcasted_iota(jnp.int32, (slots, slot_row.shape[1]), 0)
    return jnp.where(slot_row[...] == at, 1.0, 0.0).astype(BF)


def early_kernel(slot_row, wout_ref, og_ref, dgated_ref, res_ref):
    slots = res_ref.shape[0]
    dgated_ref[...] = mm_t(og_ref[...], wout_ref[...]).astype(BF)
    res_ref[...] = mm(one_hot_rows(slot_row, slots), og_ref[...])


def first_kernel(len_ref, slot_row, slot_col, rows_ref, win_ref, wout_ref, og_ref, dgated_ref, *refs):
    count = len(GROUPS)
    out_ref, wg_ref, nt_ref, dpre_ref = refs[:4]
    vqk, datt, dsil = (refs[4 + k * count : 4 + (k + 1) * count] for k in range(3))
    hid, gate, ev, att, gated, dgate, dsil_gate = refs[4 + 3 * count :]
    slots, width = rows_ref.shape
    tokens = og_ref.shape[0]
    head = width // HEADS
    half_scale = 0.5 * head**-0.5
    normed, _ = center_rows(rows_ref[...].astype(F32))
    normed = normed.astype(BF)
    nt_ref[...] = normed.T
    for j in range(4):
        cols = slice(j * width, (j + 1) * width)
        pre = mm(normed, win_ref[:, cols])
        sig = 0.5 + 0.5 * jnp.tanh(0.5 * pre)
        act = pre * sig
        hid[:, cols] = act.astype(BF)
        slope = (sig + act * (1.0 - sig)).astype(BF)
        if j == 0:
            dsil_gate[...] = slope
        else:
            for (h0, h1), ref in zip(GROUPS, dsil):
                wide = (h1 - h0) * head
                ref[:, (j - 1) * wide : j * wide] = slope[:, h0 * head : h1 * head]

    def spread(i, _):
        span = pl.ds(pl.multiple_of(i * BLOCK, BLOCK), BLOCK)
        lane = lax.broadcasted_iota(jnp.int32, (BLOCK, slots), 1)
        pick = jnp.where(slot_col[span, :] == lane, 1.0, 0.0).astype(BF)
        ev[span, :] = mm(pick, rows_ref[...]).astype(BF)
        gate[span, :] = mm(pick, hid[:, :width]).astype(BF)
        for j in range(3):
            part = mm(pick, hid[:, (j + 1) * width : (j + 2) * width]).astype(BF)
            for (h0, h1), ref in zip(GROUPS, vqk):
                wide = (h1 - h0) * head
                ref[span, j * wide : (j + 1) * wide] = part[:, h0 * head : h1 * head]
        return 0

    lax.fori_loop(0, tokens // BLOCK, spread, 0)
    ends = history_ends(len_ref)

    def rows_step(i, _):
        base = pl.multiple_of(i * BLOCK, BLOCK)
        span = pl.ds(base, BLOCK)
        start = history_start(ends, base + lax.broadcasted_iota(jnp.int32, (BLOCK, 1), 0))
        place = base + lax.broadcasted_iota(jnp.int32, (BLOCK, BLOCK), 0)
        att[...] = jnp.zeros_like(att)

        def keys_step(j, _):
            key_base = pl.multiple_of(j * BLOCK, BLOCK)
            keys = pl.ds(key_base, BLOCK)
            other = key_base + lax.broadcasted_iota(jnp.int32, (BLOCK, BLOCK), 1)
            allowed = (other >= start) & (other <= place)
            parts = []
            for (h0, h1), ref in zip(GROUPS, vqk):
                wide = (h1 - h0) * head
                for lo in range(0, wide, head):
                    q = ref[span, wide + lo : wide + lo + head]
                    k = ref[keys, 2 * wide + lo : 2 * wide + lo + head]
                    u = mm_t(q, k) * half_scale
                    w = jnp.where(allowed, u + u * jnp.tanh(u), 0.0).astype(BF)
                    parts.append(mm(w, ref[keys, lo : lo + head]))
            for h, part in enumerate(parts):
                att[:, h * head : (h + 1) * head] += part
            return 0

        lax.fori_loop(history_start(ends, base) // BLOCK, i + 1, keys_step, 0)
        normed_att, inverse = center_rows(att[...] * (1.0 / MOST))
        g = gate[span, :].astype(F32)
        gated_rows = (normed_att * g).astype(BF)
        gated[span, :] = gated_rows
        out_ref[span, :] = (mm(gated_rows, wout_ref[...]) + ev[span, :].astype(F32)).astype(BF)
        dgated = dgated_ref[span, :].astype(F32)
        dgate[span, :] = (dgated * normed_att).astype(BF)
        back = (center_back(dgated * g, normed_att, inverse) * (1.0 / MOST)).astype(BF)
        for (h0, h1), ref in zip(GROUPS, datt):
            ref[span, :] = back[:, h0 * head : h1 * head]
        return 0

    lax.fori_loop(0, tokens // BLOCK, rows_step, 0)
    wg_ref[:, :width] = tt_mm(gated[...], og_ref[...]).astype(BF)
    slot_sum = mm(one_hot_rows(slot_row, slots), dgate[...])
    dpre = (slot_sum * dsil_gate[...].astype(F32)).astype(BF)
    dpre_ref[...] = dpre
    wg_ref[:, width:] = mm(nt_ref[...], dpre).astype(BF)


def second_kernel(joined, heads, len_ref, core_ref, slot_row, vqk_ref, datt_ref, dsil_ref, nt_ref, *refs):
    before = refs[0] if joined else None
    refs = refs[1:] if joined else refs
    outs = 3 if joined else 2
    dpre_ref, sums = refs[0], refs[outs:]
    slots = dpre_ref.shape[0]
    tokens, wide = datt_ref.shape
    head = wide // heads
    half_scale = 0.5 * head**-0.5
    ends = history_ends(len_ref)
    for ref in sums:
        ref[...] = jnp.zeros_like(ref)

    def rows_step(i, _):
        base = pl.multiple_of(i * BLOCK, BLOCK)
        span = pl.ds(base, BLOCK)
        start = history_start(ends, base + lax.broadcasted_iota(jnp.int32, (1, BLOCK), 1))
        place = base + lax.broadcasted_iota(jnp.int32, (BLOCK, BLOCK), 1)

        def keys_step(j, _):
            key_base = pl.multiple_of(j * BLOCK, BLOCK)
            keys = pl.ds(key_base, BLOCK)
            other = key_base + lax.broadcasted_iota(jnp.int32, (BLOCK, BLOCK), 0)
            allowed = (other >= start) & (other <= place)
            parts = []
            for h in range(heads):
                lo = h * head
                q = vqk_ref[span, wide + lo : wide + lo + head]
                k = vqk_ref[keys, 2 * wide + lo : 2 * wide + lo + head]
                v = vqk_ref[keys, lo : lo + head]
                da = datt_ref[span, lo : lo + head]
                u = mm_t(k, q) * half_scale
                dw = mm_t(v, da)
                th = jnp.tanh(u)
                w = jnp.where(allowed, u + u * th, 0.0).astype(BF)
                slope = (half_scale + half_scale * th) * (1.0 + u - u * th)
                ds = jnp.where(allowed, dw * slope, 0.0).astype(BF)
                parts.append((mm(w, da), tt_mm(ds, k), mm(ds, q)))
            for h in range(heads):
                sums[3 * h][keys, :] += parts[h][0]
                sums[3 * h + 1][span, :] += parts[h][1]
                sums[3 * h + 2][keys, :] += parts[h][2]
            return 0

        lax.fori_loop(history_start(ends, base) // BLOCK, i + 1, keys_step, 0)
        return 0

    lax.fori_loop(0, tokens // BLOCK, rows_step, 0)
    put = one_hot_rows(slot_row, slots)
    for j in range(3):
        parts = [sums[3 * h + j][...].astype(BF) for h in range(heads)]
        cols = slice(j * wide, (j + 1) * wide)
        slot_sum = mm(put, jnp.concatenate(parts, axis=1) if heads > 1 else parts[0])
        dpre_ref[:, cols] = (slot_sum * dsil_ref[:, cols].astype(F32)).astype(BF)
    if not joined:
        refs[1][...] = mm(nt_ref[...], dpre_ref[...]).astype(BF)
        return
    half = nt_ref.shape[0] // 2
    offset = before.shape[1]
    for ref, place in ((refs[1], core_ref[0, 0]), (refs[2], 1 - core_ref[0, 0])):
        span = pl.ds(pl.multiple_of(place * half, half), half)
        ref[:, :offset] = before[span, :]
        ref[:, offset:] = mm(nt_ref[span, :], dpre_ref[...]).astype(BF)


def slot_kernel(rows_ref, res_ref, win_ref, gate_ref, *refs):
    grad_ref = refs[-1]
    width = rows_ref.shape[1]
    head = width // HEADS
    dn = mm_t(gate_ref[...], win_ref[:, :width])
    for (h0, h1), ref in zip(GROUPS, refs):
        wide = (h1 - h0) * head
        for j in range(3):
            first = (j + 1) * width + h0 * head
            dn = dn + mm_t(ref[:, j * wide : (j + 1) * wide], win_ref[:, first : first + wide])
    normed, inverse = center_rows(rows_ref[...].astype(F32))
    grad_ref[...] = (center_back(dn, normed, inverse) + res_ref[...]).astype(BF)


def assemble_kernel(core_ref, own1, got1, own2, got2, in_ref, out_ref):
    width = out_ref.shape[1]
    head = width // HEADS
    half = own1.shape[0]
    pieces = [(0, 0, out_ref, 0, width), (0, width, in_ref, 0, width)]
    at = [2 * width, 0]
    for i, (h0, h1) in enumerate(GROUPS):
        chain = 0 if i == 0 else 1
        for j in range(3):
            wide = (h1 - h0) * head
            pieces.append((chain, at[chain], in_ref, (j + 1) * width + h0 * head, wide))
            at[chain] += wide
    for sources, place in (((own1, own2), core_ref[0, 0]), ((got1, got2), 1 - core_ref[0, 0])):
        span = pl.ds(pl.multiple_of(place * half, half), half)
        for chain, source, ref, target, wide in pieces:
            ref[span, target : target + wide] = sources[chain][:, source : source + wide].astype(F32)


def table_kernel(count, *refs):
    places, rows, out = refs[:count], refs[count : 2 * count], refs[-1]
    height = min(BLOCK, out.shape[0])

    def step(i, _):
        base = pl.multiple_of(i * height, height)
        total = None
        for place, row in zip(places, rows):
            at = base + lax.broadcasted_iota(jnp.int32, (height, place.shape[1]), 0)
            put = jnp.where(place[...] == at, 1.0, 0.0).astype(BF)
            part = mm(put, row[...])
            total = part if total is None else total + part
        out[pl.ds(base, height), :] = total
        return 0

    lax.fori_loop(0, out.shape[0] // height, step, 0)


def call(kernel, outs, scratch, specs, flops, mib=24):
    return pl.pallas_call(
        kernel,
        out_shape=[jax.ShapeDtypeStruct(s, d) for s, d in outs],
        in_specs=specs,
        out_specs=[VMEM] * len(outs),
        scratch_shapes=[pltpu.VMEM(s, d) for s, d in scratch],
        compiler_params=pltpu.CompilerParams(vmem_limit_bytes=mib * 2**20),
        cost_estimate=pl.CostEstimate(flops=flops, bytes_accessed=10**7, transcendentals=0),
    )


def other_place(x, axis):
    size = lax.axis_size(axis)
    return lax.ppermute(x, axis, [(i, i ^ 1) for i in range(size)])


def exchange(x, axes):
    return lax.all_to_all(x, axes, split_axis=0, concat_axis=0, tiled=True)


def swap(x, partner):
    return lax.ppermute(x, AXES, [(d, partner(d)) for d in range(lax.axis_size(AXES))])


def weight_sum(keep, give):
    seq_bits = lax.axis_size(("s1", "s0")).bit_length() - 1
    all_bits = lax.axis_size(AXES).bit_length() - 1
    me = lax.axis_index(AXES)
    one, two = min(1, seq_bits), seq_bits
    line = [k for k in range(all_bits) if k not in (0, one, two)]
    by_core = lambda first, second: (lambda d: d ^ (1 << (second if d & 1 else first)))
    place = lambda first, second: (me >> jnp.where(me & 1 == 1, second, first)) & 1
    got = other_place(give, "s0")
    x = (keep.astype(F32) + got.astype(F32)).astype(BF)
    for first, second in ((two, one), (one, two)):
        halves = x.reshape(2, x.shape[0] // 2, x.shape[1])
        mine = lax.dynamic_index_in_dim(halves, place(first, second), 0, keepdims=False)
        give = lax.dynamic_index_in_dim(halves, 1 - place(first, second), 0, keepdims=False)
        got = swap(give, by_core(first, second))
        x = (mine.astype(F32) + got.astype(F32)).astype(BF)
    for first, second in zip(line, line[::-1]):
        got = swap(x, by_core(first, second))
        x = (x.astype(F32) + got.astype(F32)).astype(BF)
    for first, second in ((one, two), (two, one)):
        got = swap(x, by_core(first, second))
        upper = place(first, second) == 1
        x = jnp.concatenate([jnp.where(upper, got, x), jnp.where(upper, x, got)], axis=0)
    return x, other_place(x, "s0")


def on_device(item_table, fetch_rows, event_slot, lengths, in_weight, out_weight, out_grad):
    emb = ("e1", "e0")
    shard_rows, width = item_table.shape
    requests = fetch_rows.reshape(lax.axis_size(emb), -1)
    slots = requests.shape[0] * requests.shape[1]
    tokens = event_slot.shape[0]
    head = width // HEADS
    asked = exchange(requests, emb)
    found = item_table[asked]
    fetched = exchange(found, emb)
    rows = fetched.reshape(slots, width)
    slot_row, slot_col = event_slot.reshape(1, tokens), event_slot.reshape(tokens, 1)
    core = lax.axis_index("s0").reshape(1, 1)
    wides = [(h1 - h0) * head for h0, h1 in GROUPS]
    count = len(GROUPS)

    dgated, res = call(
        early_kernel, [((tokens, width), BF), ((slots, width), F32)], [], [VMEM] * 3, 10**9
    )(slot_row, out_weight, out_grad)
    outs = call(
        first_kernel,
        [((tokens, width), BF), ((width, 2 * width), BF), ((width, slots), BF), ((slots, width), BF)]
        + [((tokens, 3 * w), BF) for w in wides]
        + [((tokens, w), BF) for w in wides]
        + [((slots, 3 * w), BF) for w in wides],
        [
            ((slots, 4 * width), BF), ((tokens, width), BF), ((tokens, width), BF), ((BLOCK, width), F32),
            ((tokens, width), BF), ((tokens, width), BF), ((slots, width), BF),
        ],
        [SMEM] + [VMEM] * 7,
        10**10,
        32,
    )(lengths, slot_row, slot_col, rows, in_weight, out_weight, out_grad, dgated)
    layer_out, wg, nt, dpre_gate = outs[:4]
    vqk, datt, dsil = (outs[4 + k * count : 4 + (k + 1) * count] for k in range(3))

    def attention_back(i, before):
        heads = GROUPS[i][1] - GROUPS[i][0]
        grads = 3 * wides[i]
        joined = before is not None
        columns = grads + (before.shape[1] if joined else 0)
        return call(
            functools.partial(second_kernel, joined, heads),
            [((slots, grads), BF)]
            + ([((width // 2, columns), BF)] * 2 if joined else [((width, grads), BF)]),
            [((tokens, head), F32)] * (3 * heads),
            [SMEM] * 2 + [VMEM] * (5 + joined),
            10**9 * heads,
        )(lengths, core, slot_row, vqk[i], datt[i], dsil[i], nt, *([before] if joined else []))

    dpre_a, keep, give = attention_back(0, wg)
    own1, got1 = weight_sum(keep, give)
    dpre_b, wg_b = attention_back(1, None)
    dpre_c, keep, give = attention_back(2, wg_b)
    own2, got2 = weight_sum(keep, give)
    (slot_grad,) = call(slot_kernel, [((slots, width), BF)], [], [VMEM] * (4 + count), 10**9)(
        rows, res, in_weight, dpre_gate, dpre_a, dpre_b, dpre_c
    )

    returned = exchange(slot_grad.reshape(requests.shape + (width,)), emb)
    arrays, places = [returned.reshape(slots, width)], [asked.reshape(1, slots)]
    for axis in ("s1", "s0"):
        places += [other_place(p, axis) for p in places]
        arrays += [other_place(a, axis) for a in arrays]
    quarter = shard_rows // lax.axis_size(("s1", "s0"))
    base = lax.axis_index(("s1", "s0")) * quarter
    places = [p - base for p in places]
    (table_grad,) = call(
        functools.partial(table_kernel, len(places)),
        [((quarter, width), F32)],
        [],
        [VMEM] * (2 * len(places)),
        10**9,
    )(*places, *arrays)
    in_total, out_total = call(
        assemble_kernel,
        [((width, 4 * width), F32), ((width, width), F32)],
        [],
        [SMEM] + [VMEM] * 4,
        10**8,
    )(core, own1, got1, own2, got2)
    return layer_out, table_grad, in_total, out_total


def solution(mesh):
    emb, seq = mesh.shape["emb"], mesh.shape["seq"]
    fine = jax.sharding.Mesh(mesh.devices.reshape(emb // 2, 2, seq // 2, 2), AXES)
    placed = (
        P(("e1", "e0"), None),
        P(("e1", "e0"), ("s1", "s0"), None, None),
        P(AXES),
        P(AXES, None),
        P(),
        P(),
        P(AXES, None),
    )


    return jax.shard_map(
        on_device,
        mesh=fine,
        in_specs=placed,
        out_specs=(P(AXES, None), P(AXES, None), P(), P()),
        check_vma=False,
    )
```

```python
import functools

import jax
import jax.numpy as jnp
from jax import lax
from jax.experimental import pallas as pl
from jax.experimental.pallas import tpu as pltpu
from jax.sharding import PartitionSpec as P


HEADS = 4
MOST = 512
EPS = 1e-05
BLOCK = 256
MIB = 56
GROUPS = ((0, HEADS),)
VMEM = pl.BlockSpec(memory_space=pltpu.VMEM)
SMEM = pl.BlockSpec(memory_space=pltpu.SMEM)
BF = jnp.bfloat16
F32 = jnp.float32


AXES = ("e1", "e0", "s1", "s0")


def mm(a, b):
    return jnp.dot(a, b, preferred_element_type=F32)


def mm_t(a, b):
    return lax.dot_general(a, b, (((1,), (1,)), ((), ())), preferred_element_type=F32)


def tt_mm(a, b):
    return lax.dot_general(a, b, (((0,), (0,)), ((), ())), preferred_element_type=F32)


def center_rows(x):
    center = x - jnp.mean(x, axis=-1, keepdims=True)
    spread = jnp.mean(center * center, axis=-1, keepdims=True)
    inverse = lax.rsqrt(spread + EPS)
    return center * inverse, inverse


def center_back(grad, normed, inverse):
    along = jnp.mean(grad * normed, axis=-1, keepdims=True)
    return inverse * (grad - jnp.mean(grad, axis=-1, keepdims=True) - normed * along)


def history_ends(len_ref):
    ends, total = [], 0
    for k in range(len_ref.shape[1]):
        total = total + len_ref[0, k]
        ends.append(total)
    return ends


def history_start(ends, place):
    start = jnp.zeros_like(place)
    for end in ends:
        start = jnp.maximum(start, jnp.where(place >= end, end, 0))
    return start


def one_hot_rows(slot_row, slots):
    at = lax.broadcasted_iota(jnp.int32, (slots, slot_row.shape[1]), 0)
    return jnp.where(slot_row[...] == at, 1.0, 0.0).astype(BF)


def early_kernel(slot_row, wout_ref, og_ref, dgated_ref, res_ref):
    slots = res_ref.shape[0]
    dgated_ref[...] = mm_t(og_ref[...], wout_ref[...]).astype(BF)
    res_ref[...] = mm(one_hot_rows(slot_row, slots), og_ref[...])


def first_kernel(len_ref, slot_row, slot_col, rows_ref, win_ref, wout_ref, og_ref, dgated_ref, *refs):
    count = len(GROUPS)
    out_ref, wg_ref, nt_ref, dpre_ref = refs[:4]
    vqk, datt, dsil = (refs[4 + k * count : 4 + (k + 1) * count] for k in range(3))
    hid, gate, ev, att, gated, dgate, dsil_gate = refs[4 + 3 * count :]
    slots, width = rows_ref.shape
    tokens = og_ref.shape[0]
    head = width // HEADS
    half_scale = 0.5 * head**-0.5
    normed, _ = center_rows(rows_ref[...].astype(F32))
    normed = normed.astype(BF)
    nt_ref[...] = normed.T
    for j in range(4):
        cols = slice(j * width, (j + 1) * width)
        pre = mm(normed, win_ref[:, cols])
        sig = 0.5 + 0.5 * jnp.tanh(0.5 * pre)
        act = pre * sig
        hid[:, cols] = act.astype(BF)
        slope = (sig + act * (1.0 - sig)).astype(BF)
        if j == 0:
            dsil_gate[...] = slope
        else:
            for (h0, h1), ref in zip(GROUPS, dsil):
                wide = (h1 - h0) * head
                ref[:, (j - 1) * wide : j * wide] = slope[:, h0 * head : h1 * head]

    def spread(i, _):
        span = pl.ds(pl.multiple_of(i * BLOCK, BLOCK), BLOCK)
        lane = lax.broadcasted_iota(jnp.int32, (BLOCK, slots), 1)
        pick = jnp.where(slot_col[span, :] == lane, 1.0, 0.0).astype(BF)
        ev[span, :] = mm(pick, rows_ref[...]).astype(BF)
        gate[span, :] = mm(pick, hid[:, :width]).astype(BF)
        for j in range(3):
            part = mm(pick, hid[:, (j + 1) * width : (j + 2) * width]).astype(BF)
            for (h0, h1), ref in zip(GROUPS, vqk):
                wide = (h1 - h0) * head
                ref[span, j * wide : (j + 1) * wide] = part[:, h0 * head : h1 * head]
        return 0

    lax.fori_loop(0, tokens // BLOCK, spread, 0)
    ends = history_ends(len_ref)

    def rows_step(i, _):
        base = pl.multiple_of(i * BLOCK, BLOCK)
        span = pl.ds(base, BLOCK)
        start = history_start(ends, base + lax.broadcasted_iota(jnp.int32, (BLOCK, 1), 0))
        place = base + lax.broadcasted_iota(jnp.int32, (BLOCK, BLOCK), 0)
        att[...] = jnp.zeros_like(att)

        def keys_step(j, _):
            key_base = pl.multiple_of(j * BLOCK, BLOCK)
            keys = pl.ds(key_base, BLOCK)
            other = key_base + lax.broadcasted_iota(jnp.int32, (BLOCK, BLOCK), 1)
            allowed = (other >= start) & (other <= place)
            parts = []
            for (h0, h1), ref in zip(GROUPS, vqk):
                wide = (h1 - h0) * head
                for lo in range(0, wide, head):
                    q = ref[span, wide + lo : wide + lo + head]
                    k = ref[keys, 2 * wide + lo : 2 * wide + lo + head]
                    u = mm_t(q, k) * half_scale
                    w = jnp.where(allowed, u + u * jnp.tanh(u), 0.0).astype(BF)
                    parts.append(mm(w, ref[keys, lo : lo + head]))
            for h, part in enumerate(parts):
                att[:, h * head : (h + 1) * head] += part
            return 0

        lax.fori_loop(history_start(ends, base) // BLOCK, i + 1, keys_step, 0)
        normed_att, inverse = center_rows(att[...] * (1.0 / MOST))
        g = gate[span, :].astype(F32)
        gated_rows = (normed_att * g).astype(BF)
        gated[span, :] = gated_rows
        out_ref[span, :] = (mm(gated_rows, wout_ref[...]) + ev[span, :].astype(F32)).astype(BF)
        dgated = dgated_ref[span, :].astype(F32)
        dgate[span, :] = (dgated * normed_att).astype(BF)
        back = (center_back(dgated * g, normed_att, inverse) * (1.0 / MOST)).astype(BF)
        for (h0, h1), ref in zip(GROUPS, datt):
            ref[span, :] = back[:, h0 * head : h1 * head]
        return 0

    lax.fori_loop(0, tokens // BLOCK, rows_step, 0)
    wg_ref[:, :width] = tt_mm(gated[...], og_ref[...]).astype(BF)
    slot_sum = mm(one_hot_rows(slot_row, slots), dgate[...])
    dpre = (slot_sum * dsil_gate[...].astype(F32)).astype(BF)
    dpre_ref[...] = dpre
    wg_ref[:, width:] = mm(nt_ref[...], dpre).astype(BF)


def second_kernel(
    heads, len_ref, core_ref, slot_row, vqk_ref, datt_ref, dsil_ref, nt_ref, dpre_ref, keep_ref, give_ref, *sums
):
    slots = dpre_ref.shape[0]
    tokens, wide = datt_ref.shape
    head = wide // heads
    half_scale = 0.5 * head**-0.5
    ends = history_ends(len_ref)
    for ref in sums:
        ref[...] = jnp.zeros_like(ref)

    def rows_step(i, _):
        base = pl.multiple_of(i * BLOCK, BLOCK)
        span = pl.ds(base, BLOCK)
        start = history_start(ends, base + lax.broadcasted_iota(jnp.int32, (1, BLOCK), 1))
        place = base + lax.broadcasted_iota(jnp.int32, (BLOCK, BLOCK), 1)

        def keys_step(j, _):
            key_base = pl.multiple_of(j * BLOCK, BLOCK)
            keys = pl.ds(key_base, BLOCK)
            other = key_base + lax.broadcasted_iota(jnp.int32, (BLOCK, BLOCK), 0)
            allowed = (other >= start) & (other <= place)
            parts = []
            for h in range(heads):
                lo = h * head
                q = vqk_ref[span, wide + lo : wide + lo + head]
                k = vqk_ref[keys, 2 * wide + lo : 2 * wide + lo + head]
                v = vqk_ref[keys, lo : lo + head]
                da = datt_ref[span, lo : lo + head]
                u = mm_t(k, q) * half_scale
                dw = mm_t(v, da)
                th = jnp.tanh(u)
                w = jnp.where(allowed, u + u * th, 0.0).astype(BF)
                slope = (half_scale + half_scale * th) * (1.0 + u - u * th)
                ds = jnp.where(allowed, dw * slope, 0.0).astype(BF)
                parts.append((mm(w, da), tt_mm(ds, k), mm(ds, q)))
            for h in range(heads):
                sums[3 * h][keys, :] += parts[h][0]
                sums[3 * h + 1][span, :] += parts[h][1]
                sums[3 * h + 2][keys, :] += parts[h][2]
            return 0

        lax.fori_loop(history_start(ends, base) // BLOCK, i + 1, keys_step, 0)
        return 0

    lax.fori_loop(0, tokens // BLOCK, rows_step, 0)
    put = one_hot_rows(slot_row, slots)
    for j in range(3):
        parts = [sums[3 * h + j][...].astype(BF) for h in range(heads)]
        cols = slice(j * wide, (j + 1) * wide)
        slot_sum = mm(put, jnp.concatenate(parts, axis=1) if heads > 1 else parts[0])
        dpre_ref[:, cols] = (slot_sum * dsil_ref[:, cols].astype(F32)).astype(BF)
    half = nt_ref.shape[0] // 2
    for ref, place in ((keep_ref, core_ref[0, 0]), (give_ref, 1 - core_ref[0, 0])):
        span = pl.ds(pl.multiple_of(place * half, half), half)
        ref[...] = mm(nt_ref[span, :], dpre_ref[...]).astype(BF)


def slot_kernel(rows_ref, res_ref, win_ref, gate_ref, *refs):
    grad_ref = refs[-1]
    width = rows_ref.shape[1]
    head = width // HEADS
    dn = mm_t(gate_ref[...], win_ref[:, :width])
    for (h0, h1), ref in zip(GROUPS, refs):
        wide = (h1 - h0) * head
        for j in range(3):
            first = (j + 1) * width + h0 * head
            dn = dn + mm_t(ref[:, j * wide : (j + 1) * wide], win_ref[:, first : first + wide])
    normed, inverse = center_rows(rows_ref[...].astype(F32))
    grad_ref[...] = (center_back(dn, normed, inverse) + res_ref[...]).astype(BF)


def assemble_kernel(core_ref, early, own, got, in_ref, out_ref):
    width = out_ref.shape[1]
    half = own.shape[0]
    out_ref[...] = early[:, :width].astype(F32)
    in_ref[:, :width] = early[:, width:].astype(F32)
    for source, place in ((own, core_ref[0, 0]), (got, 1 - core_ref[0, 0])):
        span = pl.ds(pl.multiple_of(place * half, half), half)
        in_ref[span, width:] = source[...].astype(F32)


def table_kernel(count, *refs):
    places, rows, out = refs[:count], refs[count : 2 * count], refs[-1]
    height = min(BLOCK, out.shape[0])

    def step(i, _):
        base = pl.multiple_of(i * height, height)
        total = None
        for place, row in zip(places, rows):
            at = base + lax.broadcasted_iota(jnp.int32, (height, place.shape[1]), 0)
            put = jnp.where(place[...] == at, 1.0, 0.0).astype(BF)
            part = mm(put, row[...])
            total = part if total is None else total + part
        out[pl.ds(base, height), :] = total
        return 0

    lax.fori_loop(0, out.shape[0] // height, step, 0)


def call(kernel, outs, scratch, specs, flops, mib=24):
    return pl.pallas_call(
        kernel,
        out_shape=[jax.ShapeDtypeStruct(s, d) for s, d in outs],
        in_specs=specs,
        out_specs=[VMEM] * len(outs),
        scratch_shapes=[pltpu.VMEM(s, d) for s, d in scratch],
        compiler_params=pltpu.CompilerParams(vmem_limit_bytes=mib * 2**20),
        cost_estimate=pl.CostEstimate(flops=flops, bytes_accessed=10**7, transcendentals=0),
    )


def other_place(x, axis):
    size = lax.axis_size(axis)
    return lax.ppermute(x, axis, [(i, i ^ 1) for i in range(size)])


def exchange(x, axes):
    return lax.all_to_all(x, axes, split_axis=0, concat_axis=0, tiled=True)


def swap(x, partner):
    return lax.ppermute(x, AXES, [(d, partner(d)) for d in range(lax.axis_size(AXES))])


def weight_sum(keep, give):
    seq_bits = lax.axis_size(("s1", "s0")).bit_length() - 1
    all_bits = lax.axis_size(AXES).bit_length() - 1
    me = lax.axis_index(AXES)
    one, two = min(1, seq_bits), seq_bits
    line = [k for k in range(all_bits) if k not in (0, one, two)]
    by_core = lambda first, second: (lambda d: d ^ (1 << (second if d & 1 else first)))
    place = lambda first, second: (me >> jnp.where(me & 1 == 1, second, first)) & 1
    got = other_place(give, "s0")
    x = (keep.astype(F32) + got.astype(F32)).astype(BF)
    for first, second in ((two, one), (one, two)):
        halves = x.reshape(2, x.shape[0] // 2, x.shape[1])
        mine = lax.dynamic_index_in_dim(halves, place(first, second), 0, keepdims=False)
        give = lax.dynamic_index_in_dim(halves, 1 - place(first, second), 0, keepdims=False)
        got = swap(give, by_core(first, second))
        x = (mine.astype(F32) + got.astype(F32)).astype(BF)
    for first, second in zip(line, line[::-1]):
        got = swap(x, by_core(first, second))
        x = (x.astype(F32) + got.astype(F32)).astype(BF)
    for first, second in ((one, two), (two, one)):
        got = swap(x, by_core(first, second))
        upper = place(first, second) == 1
        x = jnp.concatenate([jnp.where(upper, got, x), jnp.where(upper, x, got)], axis=0)
    return x, other_place(x, "s0")


def on_device(item_table, fetch_rows, event_slot, lengths, in_weight, out_weight, out_grad):
    emb = ("e1", "e0")
    shard_rows, width = item_table.shape
    requests = fetch_rows.reshape(lax.axis_size(emb), -1)
    slots = requests.shape[0] * requests.shape[1]
    tokens = event_slot.shape[0]
    head = width // HEADS
    asked = exchange(requests, emb)
    found = item_table[asked]
    fetched = exchange(found, emb)
    rows = fetched.reshape(slots, width)
    slot_row, slot_col = event_slot.reshape(1, tokens), event_slot.reshape(tokens, 1)
    core = lax.axis_index("s0").reshape(1, 1)
    wides = [(h1 - h0) * head for h0, h1 in GROUPS]
    count = len(GROUPS)

    dgated, res = call(
        early_kernel, [((tokens, width), BF), ((slots, width), F32)], [], [VMEM] * 3, 10**9
    )(slot_row, out_weight, out_grad)
    outs = call(
        first_kernel,
        [((tokens, width), BF), ((width, 2 * width), BF), ((width, slots), BF), ((slots, width), BF)]
        + [((tokens, 3 * w), BF) for w in wides]
        + [((tokens, w), BF) for w in wides]
        + [((slots, 3 * w), BF) for w in wides],
        [
            ((slots, 4 * width), BF), ((tokens, width), BF), ((tokens, width), BF), ((BLOCK, width), F32),
            ((tokens, width), BF), ((tokens, width), BF), ((slots, width), BF),
        ],
        [SMEM] + [VMEM] * 7,
        10**10,
        MIB,
    )(lengths, slot_row, slot_col, rows, in_weight, out_weight, out_grad, dgated)
    layer_out, wg, nt, dpre_gate = outs[:4]
    vqk, datt, dsil = (outs[4 + k * count : 4 + (k + 1) * count] for k in range(3))

    heads, grads = HEADS, 3 * width
    dpre, keep, give = call(
        functools.partial(second_kernel, heads),
        [((slots, grads), BF)] + [((width // 2, grads), BF)] * 2,
        [((tokens, head), F32)] * (3 * heads),
        [SMEM] * 2 + [VMEM] * 5,
        10**10,
        MIB,
    )(lengths, core, slot_row, vqk[0], datt[0], dsil[0], nt)
    total = lax.axis_size(AXES)
    early = exchange(wg.reshape(total, width // total, 2 * width), AXES)
    early = jnp.sum(early.astype(F32), axis=0).astype(BF)
    early = jnp.broadcast_to(early[None], (total,) + early.shape)
    early = exchange(early, AXES).reshape(width, 2 * width)
    own, got = weight_sum(keep, give)
    (slot_grad,) = call(slot_kernel, [((slots, width), BF)], [], [VMEM] * (4 + count), 10**9)(
        rows, res, in_weight, dpre_gate, dpre
    )

    returned = exchange(slot_grad.reshape(requests.shape + (width,)), emb)
    arrays, places = [returned.reshape(slots, width)], [asked.reshape(1, slots)]
    for axis in ("s1", "s0"):
        places += [other_place(p, axis) for p in places]
        arrays += [other_place(a, axis) for a in arrays]
    quarter = shard_rows // lax.axis_size(("s1", "s0"))
    base = lax.axis_index(("s1", "s0")) * quarter
    places = [p - base for p in places]
    (table_grad,) = call(
        functools.partial(table_kernel, len(places)),
        [((quarter, width), F32)],
        [],
        [VMEM] * (2 * len(places)),
        10**9,
    )(*places, *arrays)
    in_total, out_total = call(
        assemble_kernel,
        [((width, 4 * width), F32), ((width, width), F32)],
        [],
        [SMEM] + [VMEM] * 3,
        10**8,
    )(core, early, own, got)
    return layer_out, table_grad, in_total, out_total


def solution(mesh):
    emb, seq = mesh.shape["emb"], mesh.shape["seq"]
    fine = jax.sharding.Mesh(mesh.devices.reshape(emb // 2, 2, seq // 2, 2), AXES)
    placed = (
        P(("e1", "e0"), None),
        P(("e1", "e0"), ("s1", "s0"), None, None),
        P(AXES),
        P(AXES, None),
        P(),
        P(),
        P(AXES, None),
    )


    return jax.shard_map(
        on_device,
        mesh=fine,
        in_specs=placed,
        out_specs=(P(AXES, None), P(AXES, None), P(), P()),
        check_vma=False,
    )
```

```python
import functools

import jax
import jax.numpy as jnp
from jax import lax
from jax.experimental import pallas as pl
from jax.experimental.pallas import tpu as pltpu
from jax.sharding import PartitionSpec as P


HEADS = 4
MOST = 512
EPS = 1e-05
BLOCK = 256
MIB = 56
GROUPS = ((0, HEADS),)
VMEM = pl.BlockSpec(memory_space=pltpu.VMEM)
SMEM = pl.BlockSpec(memory_space=pltpu.SMEM)
BF = jnp.bfloat16
F32 = jnp.float32


AXES = ("e1", "e0", "s1", "s0")


def mm(a, b):
    return jnp.dot(a, b, preferred_element_type=F32)


def mm_t(a, b):
    return lax.dot_general(a, b, (((1,), (1,)), ((), ())), preferred_element_type=F32)


def tt_mm(a, b):
    return lax.dot_general(a, b, (((0,), (0,)), ((), ())), preferred_element_type=F32)


def center_rows(x):
    center = x - jnp.mean(x, axis=-1, keepdims=True)
    spread = jnp.mean(center * center, axis=-1, keepdims=True)
    inverse = lax.rsqrt(spread + EPS)
    return center * inverse, inverse


def center_back(grad, normed, inverse):
    along = jnp.mean(grad * normed, axis=-1, keepdims=True)
    return inverse * (grad - jnp.mean(grad, axis=-1, keepdims=True) - normed * along)


def history_ends(len_ref):
    ends, total = [], 0
    for k in range(len_ref.shape[1]):
        total = total + len_ref[0, k]
        ends.append(total)
    return ends


def history_start(ends, place):
    start = jnp.zeros_like(place)
    for end in ends:
        start = jnp.maximum(start, jnp.where(place >= end, end, 0))
    return start


def one_hot_rows(slot_row, slots):
    at = lax.broadcasted_iota(jnp.int32, (slots, slot_row.shape[1]), 0)
    return jnp.where(slot_row[...] == at, 1.0, 0.0).astype(BF)


def early_kernel(slot_row, wout_ref, og_ref, dgated_ref, res_ref):
    slots = res_ref.shape[0]
    dgated_ref[...] = mm_t(og_ref[...], wout_ref[...]).astype(BF)
    res_ref[...] = mm(one_hot_rows(slot_row, slots), og_ref[...])


def blocks(ref, order, cols, value):
    rows = value.shape[0] // len(order)
    for i, block in enumerate(order):
        ref[i * rows : (i + 1) * rows, cols] = value[block * rows : (block + 1) * rows, :]


def first_kernel(order, len_ref, slot_row, slot_col, rows_ref, win_ref, wout_ref, og_ref, dgated_ref, *refs):
    count = len(GROUPS)
    out_ref, wg_ref, nt_ref, dpre_ref = refs[:4]
    vqk, datt, dsil = (refs[4 + k * count : 4 + (k + 1) * count] for k in range(3))
    hid, gate, ev, att, gated, dgate, dsil_gate = refs[4 + 3 * count :]
    slots, width = rows_ref.shape
    tokens = og_ref.shape[0]
    head = width // HEADS
    half_scale = 0.5 * head**-0.5
    normed, _ = center_rows(rows_ref[...].astype(F32))
    normed = normed.astype(BF)
    nt_ref[...] = normed.T
    for j in range(4):
        cols = slice(j * width, (j + 1) * width)
        pre = mm(normed, win_ref[:, cols])
        sig = 0.5 + 0.5 * jnp.tanh(0.5 * pre)
        act = pre * sig
        hid[:, cols] = act.astype(BF)
        slope = (sig + act * (1.0 - sig)).astype(BF)
        if j == 0:
            dsil_gate[...] = slope
        else:
            for (h0, h1), ref in zip(GROUPS, dsil):
                wide = (h1 - h0) * head
                ref[:, (j - 1) * wide : j * wide] = slope[:, h0 * head : h1 * head]

    def spread(i, _):
        span = pl.ds(pl.multiple_of(i * BLOCK, BLOCK), BLOCK)
        lane = lax.broadcasted_iota(jnp.int32, (BLOCK, slots), 1)
        pick = jnp.where(slot_col[span, :] == lane, 1.0, 0.0).astype(BF)
        ev[span, :] = mm(pick, rows_ref[...]).astype(BF)
        gate[span, :] = mm(pick, hid[:, :width]).astype(BF)
        for j in range(3):
            part = mm(pick, hid[:, (j + 1) * width : (j + 2) * width]).astype(BF)
            for (h0, h1), ref in zip(GROUPS, vqk):
                wide = (h1 - h0) * head
                ref[span, j * wide : (j + 1) * wide] = part[:, h0 * head : h1 * head]
        return 0

    lax.fori_loop(0, tokens // BLOCK, spread, 0)
    ends = history_ends(len_ref)

    def rows_step(i, _):
        base = pl.multiple_of(i * BLOCK, BLOCK)
        span = pl.ds(base, BLOCK)
        start = history_start(ends, base + lax.broadcasted_iota(jnp.int32, (BLOCK, 1), 0))
        place = base + lax.broadcasted_iota(jnp.int32, (BLOCK, BLOCK), 0)
        att[...] = jnp.zeros_like(att)

        def keys_step(j, _):
            key_base = pl.multiple_of(j * BLOCK, BLOCK)
            keys = pl.ds(key_base, BLOCK)
            other = key_base + lax.broadcasted_iota(jnp.int32, (BLOCK, BLOCK), 1)
            allowed = (other >= start) & (other <= place)
            parts = []
            for (h0, h1), ref in zip(GROUPS, vqk):
                wide = (h1 - h0) * head
                for lo in range(0, wide, head):
                    q = ref[span, wide + lo : wide + lo + head]
                    k = ref[keys, 2 * wide + lo : 2 * wide + lo + head]
                    u = mm_t(q, k) * half_scale
                    w = jnp.where(allowed, u + u * jnp.tanh(u), 0.0).astype(BF)
                    parts.append(mm(w, ref[keys, lo : lo + head]))
            for h, part in enumerate(parts):
                att[:, h * head : (h + 1) * head] += part
            return 0

        lax.fori_loop(history_start(ends, base) // BLOCK, i + 1, keys_step, 0)
        normed_att, inverse = center_rows(att[...] * (1.0 / MOST))
        g = gate[span, :].astype(F32)
        gated_rows = (normed_att * g).astype(BF)
        gated[span, :] = gated_rows
        out_ref[span, :] = (mm(gated_rows, wout_ref[...]) + ev[span, :].astype(F32)).astype(BF)
        dgated = dgated_ref[span, :].astype(F32)
        dgate[span, :] = (dgated * normed_att).astype(BF)
        back = (center_back(dgated * g, normed_att, inverse) * (1.0 / MOST)).astype(BF)
        for (h0, h1), ref in zip(GROUPS, datt):
            ref[span, :] = back[:, h0 * head : h1 * head]
        return 0

    lax.fori_loop(0, tokens // BLOCK, rows_step, 0)
    blocks(wg_ref, order, slice(0, width), tt_mm(gated[...], og_ref[...]).astype(BF))
    slot_sum = mm(one_hot_rows(slot_row, slots), dgate[...])
    dpre = (slot_sum * dsil_gate[...].astype(F32)).astype(BF)
    dpre_ref[...] = dpre
    blocks(wg_ref, order, slice(width, 2 * width), mm(nt_ref[...], dpre).astype(BF))


def second_kernel(
    heads, len_ref, core_ref, slot_row, vqk_ref, datt_ref, dsil_ref, nt_ref, dpre_ref, keep_ref, give_ref, *sums
):
    slots = dpre_ref.shape[0]
    tokens, wide = datt_ref.shape
    head = wide // heads
    half_scale = 0.5 * head**-0.5
    ends = history_ends(len_ref)
    for ref in sums:
        ref[...] = jnp.zeros_like(ref)

    def rows_step(i, _):
        base = pl.multiple_of(i * BLOCK, BLOCK)
        span = pl.ds(base, BLOCK)
        start = history_start(ends, base + lax.broadcasted_iota(jnp.int32, (1, BLOCK), 1))
        place = base + lax.broadcasted_iota(jnp.int32, (BLOCK, BLOCK), 1)

        def keys_step(j, _):
            key_base = pl.multiple_of(j * BLOCK, BLOCK)
            keys = pl.ds(key_base, BLOCK)
            other = key_base + lax.broadcasted_iota(jnp.int32, (BLOCK, BLOCK), 0)
            allowed = (other >= start) & (other <= place)
            parts = []
            for h in range(heads):
                lo = h * head
                q = vqk_ref[span, wide + lo : wide + lo + head]
                k = vqk_ref[keys, 2 * wide + lo : 2 * wide + lo + head]
                v = vqk_ref[keys, lo : lo + head]
                da = datt_ref[span, lo : lo + head]
                u = mm_t(k, q) * half_scale
                dw = mm_t(v, da)
                th = jnp.tanh(u)
                w = jnp.where(allowed, u + u * th, 0.0).astype(BF)
                slope = (half_scale + half_scale * th) * (1.0 + u - u * th)
                ds = jnp.where(allowed, dw * slope, 0.0).astype(BF)
                parts.append((mm(w, da), tt_mm(ds, k), mm(ds, q)))
            for h in range(heads):
                sums[3 * h][keys, :] += parts[h][0]
                sums[3 * h + 1][span, :] += parts[h][1]
                sums[3 * h + 2][keys, :] += parts[h][2]
            return 0

        lax.fori_loop(history_start(ends, base) // BLOCK, i + 1, keys_step, 0)
        return 0

    lax.fori_loop(0, tokens // BLOCK, rows_step, 0)
    put = one_hot_rows(slot_row, slots)
    for j in range(3):
        parts = [sums[3 * h + j][...].astype(BF) for h in range(heads)]
        cols = slice(j * wide, (j + 1) * wide)
        slot_sum = mm(put, jnp.concatenate(parts, axis=1) if heads > 1 else parts[0])
        dpre_ref[:, cols] = (slot_sum * dsil_ref[:, cols].astype(F32)).astype(BF)
    half = nt_ref.shape[0] // 2
    for ref, place in ((keep_ref, core_ref[0, 0]), (give_ref, 1 - core_ref[0, 0])):
        span = pl.ds(pl.multiple_of(place * half, half), half)
        ref[...] = mm(nt_ref[span, :], dpre_ref[...]).astype(BF)


def slot_kernel(rows_ref, res_ref, win_ref, gate_ref, *refs):
    grad_ref = refs[-1]
    width = rows_ref.shape[1]
    head = width // HEADS
    dn = mm_t(gate_ref[...], win_ref[:, :width])
    for (h0, h1), ref in zip(GROUPS, refs):
        wide = (h1 - h0) * head
        for j in range(3):
            first = (j + 1) * width + h0 * head
            dn = dn + mm_t(ref[:, j * wide : (j + 1) * wide], win_ref[:, first : first + wide])
    normed, inverse = center_rows(rows_ref[...].astype(F32))
    grad_ref[...] = (center_back(dn, normed, inverse) + res_ref[...]).astype(BF)


def assemble_kernel(core_ref, own, got, in_ref, out_ref):
    width = out_ref.shape[1]
    half = own.shape[0]
    for source, place in ((own, core_ref[0, 0]), (got, 1 - core_ref[0, 0])):
        span = pl.ds(pl.multiple_of(place * half, half), half)
        out_ref[span, :] = source[:, :width].astype(F32)
        in_ref[span, :] = source[:, width:].astype(F32)


def table_kernel(count, *refs):
    places, rows, out = refs[:count], refs[count : 2 * count], refs[-1]
    height = min(BLOCK, out.shape[0])

    def step(i, _):
        base = pl.multiple_of(i * height, height)
        total = None
        for place, row in zip(places, rows):
            at = base + lax.broadcasted_iota(jnp.int32, (height, place.shape[1]), 0)
            put = jnp.where(place[...] == at, 1.0, 0.0).astype(BF)
            part = mm(put, row[...])
            total = part if total is None else total + part
        out[pl.ds(base, height), :] = total
        return 0

    lax.fori_loop(0, out.shape[0] // height, step, 0)


def call(kernel, outs, scratch, specs, flops, mib=MIB):
    return pl.pallas_call(
        kernel,
        out_shape=[jax.ShapeDtypeStruct(s, d) for s, d in outs],
        in_specs=specs,
        out_specs=[VMEM] * len(outs),
        scratch_shapes=[pltpu.VMEM(s, d) for s, d in scratch],
        compiler_params=pltpu.CompilerParams(vmem_limit_bytes=mib * 2**20),
        cost_estimate=pl.CostEstimate(flops=flops, bytes_accessed=10**7, transcendentals=0),
    )


def other_place(x, axis):
    size = lax.axis_size(axis)
    return lax.ppermute(x, axis, [(i, i ^ 1) for i in range(size)])


def exchange(x, axes):
    return lax.all_to_all(x, axes, split_axis=0, concat_axis=0, tiled=True)


def swap(x, partner):
    return lax.ppermute(x, AXES, [(d, partner(d)) for d in range(lax.axis_size(AXES))])


def block_order():
    line = lax.axis_size("e1")
    order = []
    for d in range(lax.axis_size(AXES)):
        core, near, far = d & 1, (d >> 1) & 1, (d >> 2) & 1
        first, second = (near, far) if core else (far, near)
        order.append(((core * 2 + first) * 2 + second) * line + (d >> 3))
    return order


def weight_sum(early, keep, give):
    total, line = lax.axis_size(AXES), lax.axis_size("e1")
    me = lax.axis_index(AXES)
    early = exchange(early.reshape(total, early.shape[0] // total, early.shape[1]), AXES)
    early = jnp.sum(early.astype(F32), axis=0).astype(BF)
    early = exchange(jnp.broadcast_to(early[None], (line,) + early.shape), ("e1",))
    early = early.reshape(-1, early.shape[-1])

    by_core = lambda first, second: (lambda d: d ^ (1 << (second if d & 1 else first)))
    upper = lambda first, second: (me >> jnp.where(me & 1 == 1, second, first)) & 1
    got = other_place(give, "s0")
    x = (keep.astype(F32) + got.astype(F32)).astype(BF)
    for first, second in ((2, 1), (1, 2)):
        halves = x.reshape(2, x.shape[0] // 2, x.shape[1])
        place = upper(first, second)
        mine = lax.dynamic_index_in_dim(halves, place, 0, keepdims=False)
        give = lax.dynamic_index_in_dim(halves, 1 - place, 0, keepdims=False)
        got = swap(give, by_core(first, second))
        x = (mine.astype(F32) + got.astype(F32)).astype(BF)
    bits = range(3, total.bit_length() - 1)
    for first, second in zip(bits, bits[::-1]):
        got = swap(x, by_core(first, second))
        x = (x.astype(F32) + got.astype(F32)).astype(BF)
    x = jnp.concatenate([early, x], axis=1)
    for first, second in ((1, 2), (2, 1)):
        got = swap(x, by_core(first, second))
        place = upper(first, second) == 1
        x = jnp.concatenate([jnp.where(place, got, x), jnp.where(place, x, got)], axis=0)
    return x, other_place(x, "s0")


def on_device(item_table, fetch_rows, event_slot, lengths, in_weight, out_weight, out_grad):
    emb = ("e1", "e0")
    shard_rows, width = item_table.shape
    requests = fetch_rows.reshape(lax.axis_size(emb), -1)
    slots = requests.shape[0] * requests.shape[1]
    tokens = event_slot.shape[0]
    head = width // HEADS
    asked = exchange(requests, emb)
    found = item_table[asked]
    fetched = exchange(found, emb)
    rows = fetched.reshape(slots, width)
    slot_row, slot_col = event_slot.reshape(1, tokens), event_slot.reshape(tokens, 1)
    core = lax.axis_index("s0").reshape(1, 1)
    wides = [(h1 - h0) * head for h0, h1 in GROUPS]
    count = len(GROUPS)

    dgated, res = call(
        early_kernel, [((tokens, width), BF), ((slots, width), F32)], [], [VMEM] * 3, 10**9
    )(slot_row, out_weight, out_grad)
    first = call(
        functools.partial(first_kernel, block_order()),
        [((tokens, width), BF), ((width, 2 * width), BF), ((width, slots), BF), ((slots, width), BF)]
        + [((tokens, 3 * w), BF) for w in wides]
        + [((tokens, w), BF) for w in wides]
        + [((slots, 3 * w), BF) for w in wides],
        [
            ((slots, 4 * width), BF), ((tokens, width), BF), ((tokens, width), BF), ((BLOCK, width), F32),
            ((tokens, width), BF), ((tokens, width), BF), ((slots, width), BF),
        ],
        [SMEM] + [VMEM] * 7,
        10**10,
    )
    outs = first(lengths, slot_row, slot_col, rows, in_weight, out_weight, out_grad, dgated)
    layer_out, wg, nt, dpre_gate = outs[:4]
    vqk, datt, dsil = (outs[4 + k * count : 4 + (k + 1) * count] for k in range(3))

    heads, grads = HEADS, 3 * width
    dpre, keep, give = call(
        functools.partial(second_kernel, heads),
        [((slots, grads), BF)] + [((width // 2, grads), BF)] * 2,
        [((tokens, head), F32)] * (3 * heads),
        [SMEM] * 2 + [VMEM] * 5,
        10**10,
    )(lengths, core, slot_row, vqk[0], datt[0], dsil[0], nt)
    own, got = weight_sum(wg, keep, give)
    (slot_grad,) = call(slot_kernel, [((slots, width), BF)], [], [VMEM] * (4 + count), 10**9)(
        rows, res, in_weight, dpre_gate, dpre
    )

    returned = exchange(slot_grad.reshape(requests.shape + (width,)), emb)
    arrays, places = [returned.reshape(slots, width)], [asked.reshape(1, slots)]
    for axis in ("s1", "s0"):
        places += [other_place(p, axis) for p in places]
        arrays += [other_place(a, axis) for a in arrays]
    quarter = shard_rows // lax.axis_size(("s1", "s0"))
    base = lax.axis_index(("s1", "s0")) * quarter
    places = [p - base for p in places]
    (table_grad,) = call(
        functools.partial(table_kernel, len(places)),
        [((quarter, width), F32)],
        [],
        [VMEM] * (2 * len(places)),
        10**9,
    )(*places, *arrays)
    in_total, out_total = call(
        assemble_kernel,
        [((width, 4 * width), F32), ((width, width), F32)],
        [],
        [SMEM] + [VMEM] * 2,
        10**8,
    )(core, own, got)
    return layer_out, table_grad, in_total, out_total


def solution(mesh):
    emb, seq = mesh.shape["emb"], mesh.shape["seq"]
    fine = jax.sharding.Mesh(mesh.devices.reshape(emb // 2, 2, seq // 2, 2), AXES)
    placed = (
        P(("e1", "e0"), None),
        P(("e1", "e0"), ("s1", "s0"), None, None),
        P(AXES),
        P(AXES, None),
        P(),
        P(),
        P(AXES, None),
    )


    return jax.shard_map(
        on_device,
        mesh=fine,
        in_specs=placed,
        out_specs=(P(AXES, None), P(AXES, None), P(), P()),
        check_vma=False,
    )
```

```python
import functools

import jax
import jax.numpy as jnp
from jax import lax
from jax.experimental import pallas as pl
from jax.experimental.pallas import tpu as pltpu
from jax.sharding import PartitionSpec as P


HEADS = 4
MOST = 512
EPS = 1e-05
BLOCK = 256
MIB = 56
GROUPS = ((0, HEADS),)
VMEM = pl.BlockSpec(memory_space=pltpu.VMEM)
SMEM = pl.BlockSpec(memory_space=pltpu.SMEM)
BF = jnp.bfloat16
F32 = jnp.float32


AXES = ("e1", "e0", "s1", "s0")
PLANE = AXES[1:]


def mm(a, b):
    return jnp.dot(a, b, preferred_element_type=F32)


def mm_t(a, b):
    return lax.dot_general(a, b, (((1,), (1,)), ((), ())), preferred_element_type=F32)


def tt_mm(a, b):
    return lax.dot_general(a, b, (((0,), (0,)), ((), ())), preferred_element_type=F32)


def center_rows(x):
    center = x - jnp.mean(x, axis=-1, keepdims=True)
    spread = jnp.mean(center * center, axis=-1, keepdims=True)
    inverse = lax.rsqrt(spread + EPS)
    return center * inverse, inverse


def center_back(grad, normed, inverse):
    along = jnp.mean(grad * normed, axis=-1, keepdims=True)
    return inverse * (grad - jnp.mean(grad, axis=-1, keepdims=True) - normed * along)


def history_ends(len_ref):
    ends, total = [], 0
    for k in range(len_ref.shape[1]):
        total = total + len_ref[0, k]
        ends.append(total)
    return ends


def history_start(ends, place):
    start = jnp.zeros_like(place)
    for end in ends:
        start = jnp.maximum(start, jnp.where(place >= end, end, 0))
    return start


def one_hot_rows(slot_row, slots):
    at = lax.broadcasted_iota(jnp.int32, (slots, slot_row.shape[1]), 0)
    return jnp.where(slot_row[...] == at, 1.0, 0.0).astype(BF)


def early_kernel(slot_row, wout_ref, og_ref, dgated_ref, res_ref):
    slots = res_ref.shape[0]
    dgated_ref[...] = mm_t(og_ref[...], wout_ref[...]).astype(BF)
    res_ref[...] = mm(one_hot_rows(slot_row, slots), og_ref[...])


def blocks(ref, order, cols, value):
    rows = value.shape[0] // len(order)
    for i, block in enumerate(order):
        ref[i * rows : (i + 1) * rows, cols] = value[block * rows : (block + 1) * rows, :]


def first_kernel(order, len_ref, slot_row, slot_col, rows_ref, win_ref, wout_ref, og_ref, dgated_ref, *refs):
    count = len(GROUPS)
    out_ref, wg_ref, nt_ref, dpre_ref = refs[:4]
    vqk, datt, dsil = (refs[4 + k * count : 4 + (k + 1) * count] for k in range(3))
    hid, gate, ev, att, gated, dgate, dsil_gate = refs[4 + 3 * count :]
    slots, width = rows_ref.shape
    tokens = og_ref.shape[0]
    head = width // HEADS
    half_scale = 0.5 * head**-0.5
    normed, _ = center_rows(rows_ref[...].astype(F32))
    normed = normed.astype(BF)
    nt_ref[...] = normed.T
    for j in range(4):
        cols = slice(j * width, (j + 1) * width)
        pre = mm(normed, win_ref[:, cols])
        sig = 0.5 + 0.5 * jnp.tanh(0.5 * pre)
        act = pre * sig
        hid[:, cols] = act.astype(BF)
        slope = (sig + act * (1.0 - sig)).astype(BF)
        if j == 0:
            dsil_gate[...] = slope
        else:
            for (h0, h1), ref in zip(GROUPS, dsil):
                wide = (h1 - h0) * head
                ref[:, (j - 1) * wide : j * wide] = slope[:, h0 * head : h1 * head]

    def spread(i, _):
        span = pl.ds(pl.multiple_of(i * BLOCK, BLOCK), BLOCK)
        lane = lax.broadcasted_iota(jnp.int32, (BLOCK, slots), 1)
        pick = jnp.where(slot_col[span, :] == lane, 1.0, 0.0).astype(BF)
        ev[span, :] = mm(pick, rows_ref[...]).astype(BF)
        gate[span, :] = mm(pick, hid[:, :width]).astype(BF)
        for j in range(3):
            part = mm(pick, hid[:, (j + 1) * width : (j + 2) * width]).astype(BF)
            for (h0, h1), ref in zip(GROUPS, vqk):
                wide = (h1 - h0) * head
                ref[span, j * wide : (j + 1) * wide] = part[:, h0 * head : h1 * head]
        return 0

    lax.fori_loop(0, tokens // BLOCK, spread, 0)
    ends = history_ends(len_ref)

    def rows_step(i, _):
        base = pl.multiple_of(i * BLOCK, BLOCK)
        span = pl.ds(base, BLOCK)
        start = history_start(ends, base + lax.broadcasted_iota(jnp.int32, (BLOCK, 1), 0))
        place = base + lax.broadcasted_iota(jnp.int32, (BLOCK, BLOCK), 0)
        att[...] = jnp.zeros_like(att)

        def keys_step(j, _):
            key_base = pl.multiple_of(j * BLOCK, BLOCK)
            keys = pl.ds(key_base, BLOCK)
            other = key_base + lax.broadcasted_iota(jnp.int32, (BLOCK, BLOCK), 1)
            allowed = (other >= start) & (other <= place)
            parts = []
            for (h0, h1), ref in zip(GROUPS, vqk):
                wide = (h1 - h0) * head
                for lo in range(0, wide, head):
                    q = ref[span, wide + lo : wide + lo + head]
                    k = ref[keys, 2 * wide + lo : 2 * wide + lo + head]
                    u = mm_t(q, k) * half_scale
                    w = jnp.where(allowed, u + u * jnp.tanh(u), 0.0).astype(BF)
                    parts.append(mm(w, ref[keys, lo : lo + head]))
            for h, part in enumerate(parts):
                att[:, h * head : (h + 1) * head] += part
            return 0

        lax.fori_loop(history_start(ends, base) // BLOCK, i + 1, keys_step, 0)
        normed_att, inverse = center_rows(att[...] * (1.0 / MOST))
        g = gate[span, :].astype(F32)
        gated_rows = (normed_att * g).astype(BF)
        gated[span, :] = gated_rows
        out_ref[span, :] = (mm(gated_rows, wout_ref[...]) + ev[span, :].astype(F32)).astype(BF)
        dgated = dgated_ref[span, :].astype(F32)
        dgate[span, :] = (dgated * normed_att).astype(BF)
        back = (center_back(dgated * g, normed_att, inverse) * (1.0 / MOST)).astype(BF)
        for (h0, h1), ref in zip(GROUPS, datt):
            ref[span, :] = back[:, h0 * head : h1 * head]
        return 0

    lax.fori_loop(0, tokens // BLOCK, rows_step, 0)
    blocks(wg_ref, order, slice(0, width), tt_mm(gated[...], og_ref[...]).astype(BF))
    slot_sum = mm(one_hot_rows(slot_row, slots), dgate[...])
    dpre = (slot_sum * dsil_gate[...].astype(F32)).astype(BF)
    dpre_ref[...] = dpre
    blocks(wg_ref, order, slice(width, 2 * width), mm(nt_ref[...], dpre).astype(BF))


def second_kernel(
    heads, len_ref, core_ref, slot_row, vqk_ref, datt_ref, dsil_ref, nt_ref, dpre_ref, keep_ref, give_ref, *sums
):
    slots = dpre_ref.shape[0]
    tokens, wide = datt_ref.shape
    head = wide // heads
    half_scale = 0.5 * head**-0.5
    ends = history_ends(len_ref)
    for ref in sums:
        ref[...] = jnp.zeros_like(ref)

    def rows_step(i, _):
        base = pl.multiple_of(i * BLOCK, BLOCK)
        span = pl.ds(base, BLOCK)
        start = history_start(ends, base + lax.broadcasted_iota(jnp.int32, (1, BLOCK), 1))
        place = base + lax.broadcasted_iota(jnp.int32, (BLOCK, BLOCK), 1)

        def keys_step(j, _):
            key_base = pl.multiple_of(j * BLOCK, BLOCK)
            keys = pl.ds(key_base, BLOCK)
            other = key_base + lax.broadcasted_iota(jnp.int32, (BLOCK, BLOCK), 0)
            allowed = jnp.where((other >= start) & (other <= place), 1.0, 0.0).astype(BF)
            one, half = jnp.asarray(1.0, BF), jnp.asarray(half_scale, BF)
            parts = []
            for h in range(heads):
                lo = h * head
                q = vqk_ref[span, wide + lo : wide + lo + head]
                k = vqk_ref[keys, 2 * wide + lo : 2 * wide + lo + head]
                v = vqk_ref[keys, lo : lo + head]
                da = datt_ref[span, lo : lo + head]
                u = (mm_t(k, q) * half_scale).astype(BF)
                dw = mm_t(v, da).astype(BF) * allowed
                th = jnp.tanh(u)
                uth = u * th
                w = (u + uth) * allowed
                ds = dw * ((half + half * th) * (one + (u - uth)))
                parts.append((mm(w, da), tt_mm(ds, k), mm(ds, q)))
            for h in range(heads):
                sums[3 * h][keys, :] += parts[h][0]
                sums[3 * h + 1][span, :] += parts[h][1]
                sums[3 * h + 2][keys, :] += parts[h][2]
            return 0

        lax.fori_loop(history_start(ends, base) // BLOCK, i + 1, keys_step, 0)
        return 0

    lax.fori_loop(0, tokens // BLOCK, rows_step, 0)
    put = one_hot_rows(slot_row, slots)
    for j in range(3):
        parts = [sums[3 * h + j][...].astype(BF) for h in range(heads)]
        cols = slice(j * wide, (j + 1) * wide)
        slot_sum = mm(put, jnp.concatenate(parts, axis=1) if heads > 1 else parts[0])
        dpre_ref[:, cols] = (slot_sum * dsil_ref[:, cols].astype(F32)).astype(BF)
    half = nt_ref.shape[0] // 2
    for ref, place in ((keep_ref, core_ref[0, 0]), (give_ref, 1 - core_ref[0, 0])):
        span = pl.ds(pl.multiple_of(place * half, half), half)
        ref[...] = mm(nt_ref[span, :], dpre_ref[...]).astype(BF)


def slot_kernel(rows_ref, res_ref, win_ref, gate_ref, *refs):
    grad_ref = refs[-1]
    width = rows_ref.shape[1]
    head = width // HEADS
    dn = mm_t(gate_ref[...], win_ref[:, :width])
    for (h0, h1), ref in zip(GROUPS, refs):
        wide = (h1 - h0) * head
        for j in range(3):
            first = (j + 1) * width + h0 * head
            dn = dn + mm_t(ref[:, j * wide : (j + 1) * wide], win_ref[:, first : first + wide])
    normed, inverse = center_rows(rows_ref[...].astype(F32))
    grad_ref[...] = (center_back(dn, normed, inverse) + res_ref[...]).astype(BF)


def lay_kernel(place_ref, source, *refs):
    in_ref, out_ref = refs[-2:]
    width = out_ref.shape[1]
    out_ref[...] = source[:, :width].astype(F32)
    in_ref[...] = source[:, width:].astype(F32)


def table_kernel(count, *refs):
    places, rows, out = refs[:count], refs[count : 2 * count], refs[-1]
    height = min(BLOCK, out.shape[0])

    def step(i, _):
        base = pl.multiple_of(i * height, height)
        total = None
        for place, row in zip(places, rows):
            at = base + lax.broadcasted_iota(jnp.int32, (height, place.shape[1]), 0)
            put = jnp.where(place[...] == at, 1.0, 0.0).astype(BF)
            part = mm(put, row[...])
            total = part if total is None else total + part
        out[pl.ds(base, height), :] = total
        return 0

    lax.fori_loop(0, out.shape[0] // height, step, 0)


def call(kernel, outs, scratch, specs, flops, mib=MIB):
    return pl.pallas_call(
        kernel,
        out_shape=[jax.ShapeDtypeStruct(s, d) for s, d in outs],
        in_specs=specs,
        out_specs=[VMEM] * len(outs),
        scratch_shapes=[pltpu.VMEM(s, d) for s, d in scratch],
        compiler_params=pltpu.CompilerParams(vmem_limit_bytes=mib * 2**20),
        cost_estimate=pl.CostEstimate(flops=flops, bytes_accessed=10**7, transcendentals=0),
    )


def call_first(order, tokens, slots, width):
    wides = [(h1 - h0) * width // HEADS for h0, h1 in GROUPS]
    return call(
        functools.partial(first_kernel, order),
        [((tokens, width), BF), ((width, 2 * width), BF), ((width, slots), BF), ((slots, width), BF)]
        + [((tokens, 3 * w), BF) for w in wides]
        + [((tokens, w), BF) for w in wides]
        + [((slots, 3 * w), BF) for w in wides],
        [
            ((slots, 4 * width), BF), ((tokens, width), BF), ((tokens, width), BF), ((BLOCK, width), F32),
            ((tokens, width), BF), ((tokens, width), BF), ((slots, width), BF),
        ],
        [SMEM] + [VMEM] * 7,
        10**10,
    )


def call_attention(tokens, slots, width):
    head, grads = width // HEADS, 3 * width
    return call(
        functools.partial(second_kernel, HEADS),
        [((slots, grads), BF)] + [((width // 2, grads), BF)] * 2,
        [((tokens, head), F32)] * (3 * HEADS),
        [SMEM] * 2 + [VMEM] * 5,
        10**10,
    )


def lay(place, source, width, *into):
    half, steps = source.shape[0], 4
    rows = half // steps
    block = lambda columns: pl.BlockSpec((rows, columns), lambda i, place_ref: (place_ref[0] * steps + i, 0))
    shapes = [(2 * half, source.shape[1] - width), (2 * half, width)]
    return pl.pallas_call(
        lay_kernel,
        out_shape=[jax.ShapeDtypeStruct(s, F32) for s in shapes],
        grid_spec=pltpu.PrefetchScalarGridSpec(
            num_scalar_prefetch=1,
            grid=(steps,),
            in_specs=[pl.BlockSpec((rows, source.shape[1]), lambda i, place_ref: (i, 0))]
            + [pl.BlockSpec(memory_space=pl.ANY)] * len(into),
            out_specs=[block(shape[1]) for shape in shapes],
        ),
        input_output_aliases={2 + i: i for i in range(len(into))},
        compiler_params=pltpu.CompilerParams(vmem_limit_bytes=16 * 2**20),
        cost_estimate=pl.CostEstimate(flops=10**8, bytes_accessed=4 * 10**6, transcendentals=0),
    )(place, source, *into)


def other_place(x, axis):
    size = lax.axis_size(axis)
    return lax.ppermute(x, axis, [(i, i ^ 1) for i in range(size)])


def exchange(x, axes):
    return lax.all_to_all(x, axes, split_axis=0, concat_axis=0, tiled=True)


def swap(x, partner):
    return lax.ppermute(x, AXES, [(d, partner(d)) for d in range(lax.axis_size(AXES))])


def block_order():
    order = []
    for d in range(lax.axis_size(PLANE)):
        core, near, far = d & 1, (d >> 1) & 1, d >> 2
        first, second = (near, far) if core else (far, near)
        order.append((core * 2 + first) * 2 + second)
    return order


def weight_sum(early, keep, give):
    total, plane = lax.axis_size(AXES), lax.axis_size(PLANE)
    me = lax.axis_index(AXES)
    early = exchange(early.reshape(plane, early.shape[0] // plane, early.shape[1]), PLANE)
    early = jnp.sum(early.astype(F32), axis=0).astype(BF)
    by_core = lambda first, second: (lambda d: d ^ (1 << (second if d & 1 else first)))
    upper = lambda first, second: (me >> jnp.where(me & 1 == 1, second, first)) & 1
    got = other_place(give, "s0")
    x = (keep.astype(F32) + got.astype(F32)).astype(BF)
    for first, second in ((2, 1), (1, 2)):
        halves = x.reshape(2, x.shape[0] // 2, x.shape[1])
        place = upper(first, second)
        mine = lax.dynamic_index_in_dim(halves, place, 0, keepdims=False)
        give = lax.dynamic_index_in_dim(halves, 1 - place, 0, keepdims=False)
        got = swap(give, by_core(first, second))
        x = (mine.astype(F32) + got.astype(F32)).astype(BF)
    x = jnp.concatenate([early, x], axis=1)
    bits = range(3, total.bit_length() - 1)
    for first, second in zip(bits, bits[::-1]):
        got = swap(x, by_core(first, second))
        x = (x.astype(F32) + got.astype(F32)).astype(BF)
    for first, second in ((1, 2), (2, 1)):
        got = swap(x, by_core(first, second))
        place = upper(first, second) == 1
        x = jnp.concatenate([jnp.where(place, got, x), jnp.where(place, x, got)], axis=0)
    return x, other_place(x, "s0")


def on_device(item_table, fetch_rows, event_slot, lengths, in_weight, out_weight, out_grad):
    emb = ("e1", "e0")
    shard_rows, width = item_table.shape
    requests = fetch_rows.reshape(lax.axis_size(emb), -1)
    slots = requests.shape[0] * requests.shape[1]
    tokens = event_slot.shape[0]
    asked = exchange(requests, emb)
    found = item_table[asked]
    fetched = exchange(found, emb)
    rows = fetched.reshape(slots, width)
    slot_row, slot_col = event_slot.reshape(1, tokens), event_slot.reshape(tokens, 1)
    core = lax.axis_index("s0").reshape(1, 1)
    count = len(GROUPS)

    dgated, res = call(
        early_kernel, [((tokens, width), BF), ((slots, width), F32)], [], [VMEM] * 3, 10**9
    )(slot_row, out_weight, out_grad)
    first = call_first(block_order(), tokens, slots, width)
    outs = first(lengths, slot_row, slot_col, rows, in_weight, out_weight, out_grad, dgated)
    layer_out, wg, nt, dpre_gate = outs[:4]
    vqk, datt, dsil = (outs[4 + k * count : 4 + (k + 1) * count] for k in range(3))

    dpre, keep, give = call_attention(tokens, slots, width)(
        lengths, core, slot_row, vqk[0], datt[0], dsil[0], nt
    )
    own, got = weight_sum(wg, keep, give)
    (slot_grad,) = call(slot_kernel, [((slots, width), BF)], [], [VMEM] * (4 + count), 10**9)(
        rows, res, in_weight, dpre_gate, dpre
    )

    returned = exchange(slot_grad.reshape(requests.shape + (width,)), emb)
    arrays, places = [returned.reshape(slots, width)], [asked.reshape(1, slots)]
    for axis in ("s1", "s0"):
        places += [other_place(p, axis) for p in places]
        arrays += [other_place(a, axis) for a in arrays]
    quarter = shard_rows // lax.axis_size(("s1", "s0"))
    base = lax.axis_index(("s1", "s0")) * quarter
    places = [p - base for p in places]
    (table_grad,) = call(
        functools.partial(table_kernel, len(places)),
        [((quarter, width), F32)],
        [],
        [VMEM] * (2 * len(places)),
        10**9,
        24,
    )(*places, *arrays)
    place = core.reshape(1)
    laid = lay(place, own, width)
    in_total, out_total = lay(1 - place, got, width, *laid)
    return layer_out, table_grad, in_total, out_total


def solution(mesh):
    emb, seq = mesh.shape["emb"], mesh.shape["seq"]
    fine = jax.sharding.Mesh(mesh.devices.reshape(emb // 2, 2, seq // 2, 2), AXES)
    placed = (
        P(("e1", "e0"), None),
        P(("e1", "e0"), ("s1", "s0"), None, None),
        P(AXES),
        P(AXES, None),
        P(),
        P(),
        P(AXES, None),
    )


    return jax.shard_map(
        on_device,
        mesh=fine,
        in_specs=placed,
        out_specs=(P(AXES, None), P(AXES, None), P(), P()),
        check_vma=False,
    )
```

```python
import functools

import jax
import jax.numpy as jnp
from jax import lax
from jax.experimental import pallas as pl
from jax.experimental.pallas import tpu as pltpu
from jax.sharding import PartitionSpec as P


HEADS = 4
MOST = 512
EPS = 1e-05
BLOCK = 256
MIB = 56
GROUPS = ((0, HEADS),)
VMEM = pl.BlockSpec(memory_space=pltpu.VMEM)
SMEM = pl.BlockSpec(memory_space=pltpu.SMEM)
ANY = pl.BlockSpec(memory_space=pl.ANY)
BF = jnp.bfloat16
F32 = jnp.float32


AXES = ("e1", "e0", "s1", "s0")
PLANE = AXES[1:]


def mm(a, b):
    return jnp.dot(a, b, preferred_element_type=F32)


def mm_t(a, b):
    return lax.dot_general(a, b, (((1,), (1,)), ((), ())), preferred_element_type=F32)


def tt_mm(a, b):
    return lax.dot_general(a, b, (((0,), (0,)), ((), ())), preferred_element_type=F32)


def center_rows(x):
    center = x - jnp.mean(x, axis=-1, keepdims=True)
    spread = jnp.mean(center * center, axis=-1, keepdims=True)
    inverse = lax.rsqrt(spread + EPS)
    return center * inverse, inverse


def center_back(grad, normed, inverse):
    along = jnp.mean(grad * normed, axis=-1, keepdims=True)
    return inverse * (grad - jnp.mean(grad, axis=-1, keepdims=True) - normed * along)


def history_ends(len_ref):
    ends, total = [], 0
    for k in range(len_ref.shape[1]):
        total = total + len_ref[0, k]
        ends.append(total)
    return ends


def history_start(ends, place):
    start = jnp.zeros_like(place)
    for end in ends:
        start = jnp.maximum(start, jnp.where(place >= end, end, 0))
    return start


def one_hot_rows(slot_row, slots):
    at = lax.broadcasted_iota(jnp.int32, (slots, slot_row.shape[1]), 0)
    return jnp.where(slot_row[...] == at, 1.0, 0.0).astype(BF)


def early_kernel(slot_row, wout_ref, og_ref, dgated_ref, res_ref):
    slots = res_ref.shape[0]
    dgated_ref[...] = mm_t(og_ref[...], wout_ref[...]).astype(BF)
    res_ref[...] = mm(one_hot_rows(slot_row, slots), og_ref[...])


def blocks(ref, order, cols, value):
    rows = value.shape[0] // len(order)
    for i, block in enumerate(order):
        ref[i * rows : (i + 1) * rows, cols] = value[block * rows : (block + 1) * rows, :]


def first_kernel(order, len_ref, slot_row, slot_col, rows_ref, *refs):
    sources, targets = refs[:4], refs[4:11]
    held, kept = refs[11:15], refs[15:22]
    hid, gate, ev, att, gated, dgate, dsil_gate, sems = refs[22:]
    loads = [pltpu.make_async_copy(sources[i], held[i], sems.at[i]) for i in range(4)]
    stores = [pltpu.make_async_copy(kept[i], targets[i], sems.at[4 + i]) for i in range(7)]
    win_ref, wout_ref, og_ref, dgated_ref = held
    out_ref, wg_ref, nt_ref, dpre_ref, vqk, datt, dsil = kept
    vqk, datt, dsil = (vqk,), (datt,), (dsil,)
    for load in loads:
        load.start()
    slots, width = rows_ref.shape
    tokens = og_ref.shape[0]
    head = width // HEADS
    half_scale = 0.5 * head**-0.5
    normed, _ = center_rows(rows_ref[...].astype(F32))
    normed = normed.astype(BF)
    nt_ref[...] = normed.T
    stores[2].start()
    loads[0].wait()
    for j in range(4):
        cols = slice(j * width, (j + 1) * width)
        pre = mm(normed, win_ref[:, cols])
        sig = 0.5 + 0.5 * jnp.tanh(0.5 * pre)
        act = pre * sig
        hid[:, cols] = act.astype(BF)
        slope = (sig + act * (1.0 - sig)).astype(BF)
        if j == 0:
            dsil_gate[...] = slope
        else:
            for (h0, h1), ref in zip(GROUPS, dsil):
                wide = (h1 - h0) * head
                ref[:, (j - 1) * wide : j * wide] = slope[:, h0 * head : h1 * head]

    stores[6].start()

    def spread(i, _):
        span = pl.ds(pl.multiple_of(i * BLOCK, BLOCK), BLOCK)
        lane = lax.broadcasted_iota(jnp.int32, (BLOCK, slots), 1)
        pick = jnp.where(slot_col[span, :] == lane, 1.0, 0.0).astype(BF)
        ev[span, :] = mm(pick, rows_ref[...]).astype(BF)
        gate[span, :] = mm(pick, hid[:, :width]).astype(BF)
        for j in range(3):
            part = mm(pick, hid[:, (j + 1) * width : (j + 2) * width]).astype(BF)
            for (h0, h1), ref in zip(GROUPS, vqk):
                wide = (h1 - h0) * head
                ref[span, j * wide : (j + 1) * wide] = part[:, h0 * head : h1 * head]
        return 0

    lax.fori_loop(0, tokens // BLOCK, spread, 0)
    stores[4].start()
    for load in loads[1:]:
        load.wait()
    ends = history_ends(len_ref)

    def rows_step(i, _):
        base = pl.multiple_of(i * BLOCK, BLOCK)
        span = pl.ds(base, BLOCK)
        start = history_start(ends, base + lax.broadcasted_iota(jnp.int32, (BLOCK, 1), 0))
        place = base + lax.broadcasted_iota(jnp.int32, (BLOCK, BLOCK), 0)
        att[...] = jnp.zeros_like(att)

        def keys_step(j, _):
            key_base = pl.multiple_of(j * BLOCK, BLOCK)
            keys = pl.ds(key_base, BLOCK)
            other = key_base + lax.broadcasted_iota(jnp.int32, (BLOCK, BLOCK), 1)
            allowed = (other >= start) & (other <= place)
            parts = []
            for (h0, h1), ref in zip(GROUPS, vqk):
                wide = (h1 - h0) * head
                for lo in range(0, wide, head):
                    q = ref[span, wide + lo : wide + lo + head]
                    k = ref[keys, 2 * wide + lo : 2 * wide + lo + head]
                    u = mm_t(q, k) * half_scale
                    w = jnp.where(allowed, u + u * jnp.tanh(u), 0.0).astype(BF)
                    parts.append(mm(w, ref[keys, lo : lo + head]))
            for h, part in enumerate(parts):
                att[:, h * head : (h + 1) * head] += part
            return 0

        lax.fori_loop(history_start(ends, base) // BLOCK, i + 1, keys_step, 0)
        normed_att, inverse = center_rows(att[...] * (1.0 / MOST))
        g = gate[span, :].astype(F32)
        gated_rows = (normed_att * g).astype(BF)
        gated[span, :] = gated_rows
        out_ref[span, :] = (mm(gated_rows, wout_ref[...]) + ev[span, :].astype(F32)).astype(BF)
        dgated = dgated_ref[span, :].astype(F32)
        dgate[span, :] = (dgated * normed_att).astype(BF)
        back = (center_back(dgated * g, normed_att, inverse) * (1.0 / MOST)).astype(BF)
        for (h0, h1), ref in zip(GROUPS, datt):
            ref[span, :] = back[:, h0 * head : h1 * head]
        return 0

    lax.fori_loop(0, tokens // BLOCK, rows_step, 0)
    stores[0].start()
    stores[5].start()
    blocks(wg_ref, order, slice(0, width), tt_mm(gated[...], og_ref[...]).astype(BF))
    slot_sum = mm(one_hot_rows(slot_row, slots), dgate[...])
    dpre = (slot_sum * dsil_gate[...].astype(F32)).astype(BF)
    dpre_ref[...] = dpre
    stores[3].start()
    blocks(wg_ref, order, slice(width, 2 * width), mm(nt_ref[...], dpre).astype(BF))
    stores[1].start()
    for store in stores:
        store.wait()


def second_kernel(len_ref, core_ref, slot_row, *refs):
    sources, targets = refs[:4], refs[4:7]
    vqk_ref, datt_ref, dsil_ref, nt_ref, dpre_ref, keep_ref, give_ref, kt = refs[7:15]
    sums, sems = refs[15:-1], refs[-1]
    heads, tokens = HEADS, datt_ref.shape[0]
    slots, wide = dpre_ref.shape[0], datt_ref.shape[1]
    head = wide // heads
    half_scale = 0.5 * head**-0.5
    steps = tokens // BLOCK

    def loads(i):
        span = pl.ds(pl.multiple_of(i * BLOCK, BLOCK), BLOCK)
        return [
            pltpu.make_async_copy(source.at[span], ref.at[span], sems.at[k * steps + i])
            for k, (source, ref) in enumerate(((sources[0], vqk_ref), (sources[1], datt_ref)))
        ]

    late = [
        pltpu.make_async_copy(source, ref, sems.at[2 * steps + k])
        for k, (source, ref) in enumerate(((sources[2], dsil_ref), (sources[3], nt_ref)))
    ]
    stores = [
        pltpu.make_async_copy(ref, target, sems.at[2 * steps + 2 + k])
        for k, (ref, target) in enumerate(zip((dpre_ref, keep_ref, give_ref), targets))
    ]
    for i in range(steps):
        for load in loads(i):
            load.start()
    for load in late:
        load.start()
    ends = history_ends(len_ref)
    for ref in sums:
        ref[...] = jnp.zeros_like(ref)

    def rows_step(i, _):
        base = pl.multiple_of(i * BLOCK, BLOCK)
        span = pl.ds(base, BLOCK)
        for load in loads(i):
            load.wait()
        kt[:, span] = vqk_ref[span, 2 * wide :].T
        start = history_start(ends, base + lax.broadcasted_iota(jnp.int32, (1, BLOCK), 1))
        place = base + lax.broadcasted_iota(jnp.int32, (BLOCK, BLOCK), 1)

        def keys_step(j, _):
            key_base = pl.multiple_of(j * BLOCK, BLOCK)
            keys = pl.ds(key_base, BLOCK)
            other = key_base + lax.broadcasted_iota(jnp.int32, (BLOCK, BLOCK), 0)
            allowed = jnp.where((other >= start) & (other <= place), 1.0, 0.0).astype(BF)
            one, half = jnp.asarray(1.0, BF), jnp.asarray(half_scale, BF)
            parts = []
            for h in range(heads):
                lo = h * head
                q = vqk_ref[span, wide + lo : wide + lo + head]
                k = vqk_ref[keys, 2 * wide + lo : 2 * wide + lo + head]
                v = vqk_ref[keys, lo : lo + head]
                da = datt_ref[span, lo : lo + head]
                u = (mm_t(k, q) * half_scale).astype(BF)
                dw = mm_t(v, da).astype(BF) * allowed
                th = jnp.tanh(u)
                uth = u * th
                w = (u + uth) * allowed
                ds = dw * ((half + half * th) * (one + (u - uth)))
                parts.append((mm(w, da), mm(kt[lo : lo + head, keys], ds), mm(ds, q)))
            for h in range(heads):
                sums[3 * h][keys, :] += parts[h][0]
                sums[3 * h + 1][:, span] += parts[h][1]
                sums[3 * h + 2][keys, :] += parts[h][2]
            return 0

        lax.fori_loop(history_start(ends, base) // BLOCK, i + 1, keys_step, 0)
        return 0

    lax.fori_loop(0, steps, rows_step, 0)
    put = one_hot_rows(slot_row, slots)
    for load in late:
        load.wait()
    for j in range(3):
        parts = [sums[3 * h + j][...].astype(BF) for h in range(heads)]
        cols = slice(j * wide, (j + 1) * wide)
        if j == 1:
            slot_sum = mm_t(put, jnp.concatenate(parts, axis=0))
        else:
            slot_sum = mm(put, jnp.concatenate(parts, axis=1))
        dpre_ref[:, cols] = (slot_sum * dsil_ref[:, cols].astype(F32)).astype(BF)
    stores[0].start()
    half = nt_ref.shape[0] // 2
    for k, ref, place in ((2, give_ref, 1 - core_ref[0, 0]), (1, keep_ref, core_ref[0, 0])):
        span = pl.ds(pl.multiple_of(place * half, half), half)
        ref[...] = mm(nt_ref[span, :], dpre_ref[...]).astype(BF)
        stores[k].start()
    for store in stores:
        store.wait()


def slot_kernel(rows_ref, res_ref, win_ref, gate_ref, *refs):
    grad_ref = refs[-1]
    width = rows_ref.shape[1]
    head = width // HEADS
    dn = mm_t(gate_ref[...], win_ref[:, :width])
    for (h0, h1), ref in zip(GROUPS, refs):
        wide = (h1 - h0) * head
        for j in range(3):
            first = (j + 1) * width + h0 * head
            dn = dn + mm_t(ref[:, j * wide : (j + 1) * wide], win_ref[:, first : first + wide])
    normed, inverse = center_rows(rows_ref[...].astype(F32))
    grad_ref[...] = (center_back(dn, normed, inverse) + res_ref[...]).astype(BF)


def lay_kernel(place_ref, source, *refs):
    in_ref, out_ref = refs[-2:]
    width = out_ref.shape[1]
    out_ref[...] = source[:, :width].astype(F32)
    in_ref[...] = source[:, width:].astype(F32)


def table_kernel(count, *refs):
    places, rows, out = refs[:count], refs[count : 2 * count], refs[-1]
    height = min(BLOCK, out.shape[0])

    def step(i, _):
        base = pl.multiple_of(i * height, height)
        total = None
        for place, row in zip(places, rows):
            at = base + lax.broadcasted_iota(jnp.int32, (height, place.shape[1]), 0)
            put = jnp.where(place[...] == at, 1.0, 0.0).astype(BF)
            part = mm(put, row[...])
            total = part if total is None else total + part
        out[pl.ds(base, height), :] = total
        return 0

    lax.fori_loop(0, out.shape[0] // height, step, 0)


def call(kernel, outs, scratch, specs, flops, mib=MIB, own_copies=0):
    semaphores = [pltpu.SemaphoreType.DMA((own_copies,))] if own_copies else []
    return pl.pallas_call(
        kernel,
        out_shape=[jax.ShapeDtypeStruct(s, d) for s, d in outs],
        in_specs=specs,
        out_specs=[ANY if own_copies else VMEM] * len(outs),
        scratch_shapes=[pltpu.VMEM(s, d) for s, d in scratch] + semaphores,
        compiler_params=pltpu.CompilerParams(vmem_limit_bytes=mib * 2**20),
        cost_estimate=pl.CostEstimate(flops=flops, bytes_accessed=10**7, transcendentals=0),
    )


def call_first(order, tokens, slots, width):
    loads = [((width, 4 * width), BF), ((width, width), BF), ((tokens, width), BF), ((tokens, width), BF)]
    outs = [
        ((tokens, width), BF), ((width, 2 * width), BF), ((width, slots), BF), ((slots, width), BF),
        ((tokens, 3 * width), BF), ((tokens, width), BF), ((slots, 3 * width), BF),
    ]
    return call(
        functools.partial(first_kernel, order),
        outs,
        loads + outs
        + [
            ((slots, 4 * width), BF), ((tokens, width), BF), ((tokens, width), BF), ((BLOCK, width), F32),
            ((tokens, width), BF), ((tokens, width), BF), ((slots, width), BF),
        ],
        [SMEM] + [VMEM] * 3 + [ANY] * 4,
        10**10,
        own_copies=len(loads) + len(outs),
    )


def call_attention(tokens, slots, width):
    head, grads = width // HEADS, 3 * width
    loads = [((tokens, grads), BF), ((tokens, width), BF), ((slots, grads), BF), ((width, slots), BF)]
    outs = [((slots, grads), BF)] + [((width // 2, grads), BF)] * 2
    sums = [((tokens, head), F32), ((head, tokens), F32), ((tokens, head), F32)] * HEADS
    return call(
        second_kernel,
        outs,
        loads + outs + [((width, tokens), BF)] + sums,
        [SMEM] * 2 + [VMEM] + [ANY] * 4,
        10**10,
        own_copies=2 * (tokens // BLOCK) + 5,
    )


def lay(place, source, width, *into):
    half, steps = source.shape[0], 4
    rows = half // steps
    block = lambda columns: pl.BlockSpec((rows, columns), lambda i, place_ref: (place_ref[0] * steps + i, 0))
    shapes = [(2 * half, source.shape[1] - width), (2 * half, width)]
    return pl.pallas_call(
        lay_kernel,
        out_shape=[jax.ShapeDtypeStruct(s, F32) for s in shapes],
        grid_spec=pltpu.PrefetchScalarGridSpec(
            num_scalar_prefetch=1,
            grid=(steps,),
            in_specs=[pl.BlockSpec((rows, source.shape[1]), lambda i, place_ref: (i, 0))]
            + [pl.BlockSpec(memory_space=pl.ANY)] * len(into),
            out_specs=[block(shape[1]) for shape in shapes],
        ),
        input_output_aliases={2 + i: i for i in range(len(into))},
        compiler_params=pltpu.CompilerParams(vmem_limit_bytes=16 * 2**20),
        cost_estimate=pl.CostEstimate(flops=10**8, bytes_accessed=4 * 10**6, transcendentals=0),
    )(place, source, *into)


def other_place(x, axis):
    size = lax.axis_size(axis)
    return lax.ppermute(x, axis, [(i, i ^ 1) for i in range(size)])


def exchange(x, axes):
    return lax.all_to_all(x, axes, split_axis=0, concat_axis=0, tiled=True)


def swap(x, partner):
    return lax.ppermute(x, AXES, [(d, partner(d)) for d in range(lax.axis_size(AXES))])


def block_order():
    order = []
    for d in range(lax.axis_size(PLANE)):
        core, near, far = d & 1, (d >> 1) & 1, d >> 2
        first, second = (near, far) if core else (far, near)
        order.append((core * 2 + first) * 2 + second)
    return order


def weight_sum(early, keep, give):
    total, plane = lax.axis_size(AXES), lax.axis_size(PLANE)
    me = lax.axis_index(AXES)
    early = exchange(early.reshape(plane, early.shape[0] // plane, early.shape[1]), PLANE)
    early = jnp.sum(early.astype(F32), axis=0).astype(BF)

    by_core = lambda first, second: (lambda d: d ^ (1 << (second if d & 1 else first)))
    upper = lambda first, second: (me >> jnp.where(me & 1 == 1, second, first)) & 1
    bits = range(3, total.bit_length() - 1)

    def sum_line(x):
        for first, second in zip(bits, bits[::-1]):
            got = swap(x, by_core(first, second))
            x = (x.astype(F32) + got.astype(F32)).astype(BF)
        return x

    early = sum_line(early)
    got = other_place(give, "s0")
    x = (keep.astype(F32) + got.astype(F32)).astype(BF)
    for first, second in ((2, 1), (1, 2)):
        halves = x.reshape(2, x.shape[0] // 2, x.shape[1])
        place = upper(first, second)
        mine = lax.dynamic_index_in_dim(halves, place, 0, keepdims=False)
        give = lax.dynamic_index_in_dim(halves, 1 - place, 0, keepdims=False)
        got = swap(give, by_core(first, second))
        x = (mine.astype(F32) + got.astype(F32)).astype(BF)
    x = jnp.concatenate([early, sum_line(x)], axis=1)
    for first, second in ((1, 2), (2, 1)):
        got = swap(x, by_core(first, second))
        place = upper(first, second) == 1
        x = jnp.concatenate([jnp.where(place, got, x), jnp.where(place, x, got)], axis=0)
    return x, other_place(x, "s0")


def on_device(item_table, fetch_rows, event_slot, lengths, in_weight, out_weight, out_grad):
    emb = ("e1", "e0")
    shard_rows, width = item_table.shape
    requests = fetch_rows.reshape(lax.axis_size(emb), -1)
    slots = requests.shape[0] * requests.shape[1]
    tokens = event_slot.shape[0]
    asked = exchange(requests, emb)
    found = item_table[asked]
    fetched = exchange(found, emb)
    rows = fetched.reshape(slots, width)
    slot_row, slot_col = event_slot.reshape(1, tokens), event_slot.reshape(tokens, 1)
    core = lax.axis_index("s0").reshape(1, 1)
    count = len(GROUPS)

    dgated, res = call(
        early_kernel, [((tokens, width), BF), ((slots, width), F32)], [], [VMEM] * 3, 10**9
    )(slot_row, out_weight, out_grad)
    first = call_first(block_order(), tokens, slots, width)
    outs = first(lengths, slot_row, slot_col, rows, in_weight, out_weight, out_grad, dgated)
    layer_out, wg, nt, dpre_gate = outs[:4]
    vqk, datt, dsil = (outs[4 + k * count : 4 + (k + 1) * count] for k in range(3))

    dpre, keep, give = call_attention(tokens, slots, width)(
        lengths, core, slot_row, vqk[0], datt[0], dsil[0], nt
    )
    own, got = weight_sum(wg, keep, give)
    (slot_grad,) = call(slot_kernel, [((slots, width), BF)], [], [VMEM] * (4 + count), 10**9)(
        rows, res, in_weight, dpre_gate, dpre
    )

    returned = exchange(slot_grad.reshape(requests.shape + (width,)), emb)
    arrays, places = [returned.reshape(slots, width)], [asked.reshape(1, slots)]
    for axis in ("s1", "s0"):
        places += [other_place(p, axis) for p in places]
        arrays += [other_place(a, axis) for a in arrays]
    quarter = shard_rows // lax.axis_size(("s1", "s0"))
    base = lax.axis_index(("s1", "s0")) * quarter
    places = [p - base for p in places]
    (table_grad,) = call(
        functools.partial(table_kernel, len(places)),
        [((quarter, width), F32)],
        [],
        [VMEM] * (2 * len(places)),
        10**9,
        24,
    )(*places, *arrays)
    place = core.reshape(1)
    laid = lay(place, own, width)
    in_total, out_total = lay(1 - place, got, width, *laid)
    return layer_out, table_grad, in_total, out_total


def solution(mesh):
    emb, seq = mesh.shape["emb"], mesh.shape["seq"]
    fine = jax.sharding.Mesh(mesh.devices.reshape(emb // 2, 2, seq // 2, 2), AXES)
    placed = (
        P(("e1", "e0"), None),
        P(("e1", "e0"), ("s1", "s0"), None, None),
        P(AXES),
        P(AXES, None),
        P(),
        P(),
        P(AXES, None),
    )


    return jax.shard_map(
        on_device,
        mesh=fine,
        in_specs=placed,
        out_specs=(P(AXES, None), P(AXES, None), P(), P()),
        check_vma=False,
    )
```

```python
import functools

import jax
import jax.numpy as jnp
from jax import lax
from jax.experimental import pallas as pl
from jax.experimental.pallas import tpu as pltpu
from jax.sharding import PartitionSpec as P


HEADS = 4
MOST = 512
EPS = 1e-05
BLOCK = 256
MIB = 56
GROUPS = ((0, HEADS),)
VMEM = pl.BlockSpec(memory_space=pltpu.VMEM)
SMEM = pl.BlockSpec(memory_space=pltpu.SMEM)
ANY = pl.BlockSpec(memory_space=pl.ANY)
BF = jnp.bfloat16
F32 = jnp.float32


AXES = ("e1", "e0", "s1", "s0")
PLANE = AXES[1:]


def mm(a, b):
    return jnp.dot(a, b, preferred_element_type=F32)


def mm_t(a, b):
    return lax.dot_general(a, b, (((1,), (1,)), ((), ())), preferred_element_type=F32)


def tt_mm(a, b):
    return lax.dot_general(a, b, (((0,), (0,)), ((), ())), preferred_element_type=F32)


def center_rows(x):
    center = x - jnp.mean(x, axis=-1, keepdims=True)
    spread = jnp.mean(center * center, axis=-1, keepdims=True)
    inverse = lax.rsqrt(spread + EPS)
    return center * inverse, inverse


def center_back(grad, normed, inverse):
    along = jnp.mean(grad * normed, axis=-1, keepdims=True)
    return inverse * (grad - jnp.mean(grad, axis=-1, keepdims=True) - normed * along)


def history_ends(len_ref):
    ends, total = [], 0
    for k in range(len_ref.shape[1]):
        total = total + len_ref[0, k]
        ends.append(total)
    return ends


def history_start(ends, place):
    start = jnp.zeros_like(place)
    for end in ends:
        start = jnp.maximum(start, jnp.where(place >= end, end, 0))
    return start


def one_hot_rows(slot_row, slots):
    at = lax.broadcasted_iota(jnp.int32, (slots, slot_row.shape[1]), 0)
    return jnp.where(slot_row[...] == at, 1.0, 0.0).astype(BF)


def early_kernel(slot_row, wout_ref, og_ref, dgated_ref, res_ref):
    slots = res_ref.shape[0]
    dgated_ref[...] = mm_t(og_ref[...], wout_ref[...]).astype(BF)
    res_ref[...] = mm(one_hot_rows(slot_row, slots), og_ref[...])


def blocks(ref, order, cols, value):
    rows = value.shape[0] // len(order)
    for i, block in enumerate(order):
        ref[i * rows : (i + 1) * rows, cols] = value[block * rows : (block + 1) * rows, :]


def first_kernel(order, len_ref, slot_row, slot_col, rows_ref, *refs):
    sources, targets = refs[:4], refs[4:11]
    held, kept = refs[11:15], refs[15:22]
    hid, gate, ev, att, gated, dgate, dsil_gate, sems = refs[22:]
    loads = [pltpu.make_async_copy(sources[i], held[i], sems.at[i]) for i in range(4)]
    stores = [pltpu.make_async_copy(kept[i], targets[i], sems.at[4 + i]) for i in range(7)]
    win_ref, wout_ref, og_ref, dgated_ref = held
    out_ref, wg_ref, nt_ref, dpre_ref, vqk, datt, dsil = kept
    vqk, datt, dsil = (vqk,), (datt,), (dsil,)
    for load in loads:
        load.start()
    slots, width = rows_ref.shape
    tokens = og_ref.shape[0]
    head = width // HEADS
    half_scale = 0.5 * head**-0.5
    normed, _ = center_rows(rows_ref[...].astype(F32))
    normed = normed.astype(BF)
    nt_ref[...] = normed.T
    stores[2].start()
    loads[0].wait()
    for j in range(4):
        cols = slice(j * width, (j + 1) * width)
        pre = mm(normed, win_ref[:, cols])
        sig = 0.5 + 0.5 * jnp.tanh(0.5 * pre)
        act = pre * sig
        hid[:, cols] = act.astype(BF)
        slope = (sig + act * (1.0 - sig)).astype(BF)
        if j == 0:
            dsil_gate[...] = slope
        else:
            for (h0, h1), ref in zip(GROUPS, dsil):
                wide = (h1 - h0) * head
                ref[:, (j - 1) * wide : j * wide] = slope[:, h0 * head : h1 * head]

    stores[6].start()

    def spread(i, _):
        span = pl.ds(pl.multiple_of(i * BLOCK, BLOCK), BLOCK)
        lane = lax.broadcasted_iota(jnp.int32, (BLOCK, slots), 1)
        pick = jnp.where(slot_col[span, :] == lane, 1.0, 0.0).astype(BF)
        ev[span, :] = mm(pick, rows_ref[...]).astype(BF)
        gate[span, :] = mm(pick, hid[:, :width]).astype(BF)
        for j in range(3):
            part = mm(pick, hid[:, (j + 1) * width : (j + 2) * width]).astype(BF)
            for (h0, h1), ref in zip(GROUPS, vqk):
                wide = (h1 - h0) * head
                ref[span, j * wide : (j + 1) * wide] = part[:, h0 * head : h1 * head]
        return 0

    lax.fori_loop(0, tokens // BLOCK, spread, 0)
    stores[4].start()
    for load in loads[1:]:
        load.wait()
    ends = history_ends(len_ref)

    def rows_step(i, _):
        base = pl.multiple_of(i * BLOCK, BLOCK)
        span = pl.ds(base, BLOCK)
        start = history_start(ends, base + lax.broadcasted_iota(jnp.int32, (BLOCK, 1), 0))
        place = base + lax.broadcasted_iota(jnp.int32, (BLOCK, BLOCK), 0)
        att[...] = jnp.zeros_like(att)

        def keys_step(j, _):
            key_base = pl.multiple_of(j * BLOCK, BLOCK)
            keys = pl.ds(key_base, BLOCK)
            other = key_base + lax.broadcasted_iota(jnp.int32, (BLOCK, BLOCK), 1)
            allowed = (other >= start) & (other <= place)
            parts = []
            for (h0, h1), ref in zip(GROUPS, vqk):
                wide = (h1 - h0) * head
                for lo in range(0, wide, head):
                    q = ref[span, wide + lo : wide + lo + head]
                    k = ref[keys, 2 * wide + lo : 2 * wide + lo + head]
                    u = mm_t(q, k) * half_scale
                    w = jnp.where(allowed, u + u * jnp.tanh(u), 0.0).astype(BF)
                    parts.append(mm(w, ref[keys, lo : lo + head]))
            for h, part in enumerate(parts):
                att[:, h * head : (h + 1) * head] += part
            return 0

        lax.fori_loop(history_start(ends, base) // BLOCK, i + 1, keys_step, 0)
        normed_att, inverse = center_rows(att[...] * (1.0 / MOST))
        g = gate[span, :].astype(F32)
        gated_rows = (normed_att * g).astype(BF)
        gated[span, :] = gated_rows
        out_ref[span, :] = (mm(gated_rows, wout_ref[...]) + ev[span, :].astype(F32)).astype(BF)
        dgated = dgated_ref[span, :].astype(F32)
        dgate[span, :] = (dgated * normed_att).astype(BF)
        back = (center_back(dgated * g, normed_att, inverse) * (1.0 / MOST)).astype(BF)
        for (h0, h1), ref in zip(GROUPS, datt):
            ref[span, :] = back[:, h0 * head : h1 * head]
        return 0

    lax.fori_loop(0, tokens // BLOCK, rows_step, 0)
    stores[0].start()
    stores[5].start()
    blocks(wg_ref, order, slice(0, width), tt_mm(gated[...], og_ref[...]).astype(BF))
    slot_sum = mm(one_hot_rows(slot_row, slots), dgate[...])
    dpre = (slot_sum * dsil_gate[...].astype(F32)).astype(BF)
    dpre_ref[...] = dpre
    stores[3].start()
    blocks(wg_ref, order, slice(width, 2 * width), mm(nt_ref[...], dpre).astype(BF))
    stores[1].start()
    for store in stores:
        store.wait()


def second_kernel(len_ref, core_ref, slot_row, *refs):
    sources, targets = refs[:8], refs[8:11]
    vqk_ref, datt_ref, dsil_ref, nt_ref, win_ref, rows_ref, res_ref, gate_ref = refs[11:19]
    grad_ref, keep_ref, give_ref, dpre_ref, kt = refs[19:24]
    sums, sems = refs[24:-1], refs[-1]
    heads, tokens = HEADS, datt_ref.shape[0]
    slots, wide = dpre_ref.shape[0], datt_ref.shape[1]
    head = wide // heads
    half_scale = 0.5 * head**-0.5
    steps = tokens // BLOCK

    def loads(i):
        span = pl.ds(pl.multiple_of(i * BLOCK, BLOCK), BLOCK)
        return [
            pltpu.make_async_copy(source.at[span], ref.at[span], sems.at[k * steps + i])
            for k, (source, ref) in enumerate(((sources[0], vqk_ref), (sources[1], datt_ref)))
        ]

    late = [
        pltpu.make_async_copy(source, ref, sems.at[2 * steps + k])
        for k, (source, ref) in enumerate(zip(sources[2:], refs[13:19]))
    ]
    stores = [
        pltpu.make_async_copy(ref, target, sems.at[2 * steps + 6 + k])
        for k, (ref, target) in enumerate(zip((grad_ref, keep_ref, give_ref), targets))
    ]
    for i in range(steps):
        for load in loads(i):
            load.start()
    for load in late:
        load.start()
    ends = history_ends(len_ref)
    for ref in sums:
        ref[...] = jnp.zeros_like(ref)

    def rows_step(i, _):
        base = pl.multiple_of(i * BLOCK, BLOCK)
        span = pl.ds(base, BLOCK)
        for load in loads(i):
            load.wait()
        kt[:, span] = vqk_ref[span, 2 * wide :].T
        start = history_start(ends, base + lax.broadcasted_iota(jnp.int32, (1, BLOCK), 1))
        place = base + lax.broadcasted_iota(jnp.int32, (BLOCK, BLOCK), 1)

        def keys_step(j, _):
            key_base = pl.multiple_of(j * BLOCK, BLOCK)
            keys = pl.ds(key_base, BLOCK)
            other = key_base + lax.broadcasted_iota(jnp.int32, (BLOCK, BLOCK), 0)
            allowed = jnp.where((other >= start) & (other <= place), 1.0, 0.0).astype(BF)
            one, half = jnp.asarray(1.0, BF), jnp.asarray(half_scale, BF)
            parts = []
            for h in range(heads):
                lo = h * head
                q = vqk_ref[span, wide + lo : wide + lo + head]
                k = vqk_ref[keys, 2 * wide + lo : 2 * wide + lo + head]
                v = vqk_ref[keys, lo : lo + head]
                da = datt_ref[span, lo : lo + head]
                u = (mm_t(k, q) * half_scale).astype(BF)
                dw = mm_t(v, da).astype(BF) * allowed
                th = jnp.tanh(u)
                uth = u * th
                w = (u + uth) * allowed
                ds = dw * ((half + half * th) * (one + (u - uth)))
                parts.append((mm(w, da), mm(kt[lo : lo + head, keys], ds), mm(ds, q)))
            for h in range(heads):
                sums[3 * h][keys, :] += parts[h][0]
                sums[3 * h + 1][:, span] += parts[h][1]
                sums[3 * h + 2][keys, :] += parts[h][2]
            return 0

        lax.fori_loop(history_start(ends, base) // BLOCK, i + 1, keys_step, 0)
        return 0

    lax.fori_loop(0, steps, rows_step, 0)
    put = one_hot_rows(slot_row, slots)
    for load in late:
        load.wait()
    dn = mm_t(gate_ref[...], win_ref[:, :wide])
    for j in range(3):
        parts = [sums[3 * h + j][...].astype(BF) for h in range(heads)]
        cols = slice(j * wide, (j + 1) * wide)
        if j == 1:
            slot_sum = mm_t(put, jnp.concatenate(parts, axis=0))
        else:
            slot_sum = mm(put, jnp.concatenate(parts, axis=1))
        dpre = (slot_sum * dsil_ref[:, cols].astype(F32)).astype(BF)
        dpre_ref[:, cols] = dpre
        dn = dn + mm_t(dpre, win_ref[:, (j + 1) * wide : (j + 2) * wide])
    normed, inverse = center_rows(rows_ref[...].astype(F32))
    grad_ref[...] = (center_back(dn, normed, inverse) + res_ref[...]).astype(BF)
    stores[0].start()
    half = nt_ref.shape[0] // 2
    for k, ref, place in ((2, give_ref, 1 - core_ref[0, 0]), (1, keep_ref, core_ref[0, 0])):
        span = pl.ds(pl.multiple_of(place * half, half), half)
        ref[...] = mm(nt_ref[span, :], dpre_ref[...]).astype(BF)
        stores[k].start()
    for store in stores:
        store.wait()


def lay_kernel(place_ref, source, *refs):
    in_ref, out_ref = refs[-2:]
    width = out_ref.shape[1]
    out_ref[...] = source[:, :width].astype(F32)
    in_ref[...] = source[:, width:].astype(F32)


def table_kernel(count, *refs):
    places, rows, out = refs[:count], refs[count : 2 * count], refs[-1]
    height = min(BLOCK, out.shape[0])

    def step(i, _):
        base = pl.multiple_of(i * height, height)
        total = None
        for place, row in zip(places, rows):
            at = base + lax.broadcasted_iota(jnp.int32, (height, place.shape[1]), 0)
            put = jnp.where(place[...] == at, 1.0, 0.0).astype(BF)
            part = mm(put, row[...])
            total = part if total is None else total + part
        out[pl.ds(base, height), :] = total
        return 0

    lax.fori_loop(0, out.shape[0] // height, step, 0)


def call(kernel, outs, scratch, specs, flops, mib=MIB, own_copies=0):
    semaphores = [pltpu.SemaphoreType.DMA((own_copies,))] if own_copies else []
    return pl.pallas_call(
        kernel,
        out_shape=[jax.ShapeDtypeStruct(s, d) for s, d in outs],
        in_specs=specs,
        out_specs=[ANY if own_copies else VMEM] * len(outs),
        scratch_shapes=[pltpu.VMEM(s, d) for s, d in scratch] + semaphores,
        compiler_params=pltpu.CompilerParams(vmem_limit_bytes=mib * 2**20),
        cost_estimate=pl.CostEstimate(flops=flops, bytes_accessed=10**7, transcendentals=0),
    )


def call_first(order, tokens, slots, width):
    loads = [((width, 4 * width), BF), ((width, width), BF), ((tokens, width), BF), ((tokens, width), BF)]
    outs = [
        ((tokens, width), BF), ((width, 2 * width), BF), ((width, slots), BF), ((slots, width), BF),
        ((tokens, 3 * width), BF), ((tokens, width), BF), ((slots, 3 * width), BF),
    ]
    return call(
        functools.partial(first_kernel, order),
        outs,
        loads + outs
        + [
            ((slots, 4 * width), BF), ((tokens, width), BF), ((tokens, width), BF), ((BLOCK, width), F32),
            ((tokens, width), BF), ((tokens, width), BF), ((slots, width), BF),
        ],
        [SMEM] + [VMEM] * 3 + [ANY] * 4,
        10**10,
        own_copies=len(loads) + len(outs),
    )


def call_attention(tokens, slots, width):
    head, grads = width // HEADS, 3 * width
    loads = [
        ((tokens, grads), BF), ((tokens, width), BF), ((slots, grads), BF), ((width, slots), BF),
        ((width, 4 * width), BF), ((slots, width), BF), ((slots, width), F32), ((slots, width), BF),
    ]
    outs = [((slots, width), BF)] + [((width // 2, grads), BF)] * 2
    sums = [((tokens, head), F32), ((head, tokens), F32), ((tokens, head), F32)] * HEADS
    return call(
        second_kernel,
        outs,
        loads + outs + [((slots, grads), BF), ((width, tokens), BF)] + sums,
        [SMEM] * 2 + [VMEM] + [ANY] * 8,
        10**10,
        own_copies=2 * (tokens // BLOCK) + 9,
    )


def lay(place, source, width, *into):
    half, steps = source.shape[0], 4
    rows = half // steps
    block = lambda columns: pl.BlockSpec((rows, columns), lambda i, place_ref: (place_ref[0] * steps + i, 0))
    shapes = [(2 * half, source.shape[1] - width), (2 * half, width)]
    return pl.pallas_call(
        lay_kernel,
        out_shape=[jax.ShapeDtypeStruct(s, F32) for s in shapes],
        grid_spec=pltpu.PrefetchScalarGridSpec(
            num_scalar_prefetch=1,
            grid=(steps,),
            in_specs=[pl.BlockSpec((rows, source.shape[1]), lambda i, place_ref: (i, 0))]
            + [pl.BlockSpec(memory_space=pl.ANY)] * len(into),
            out_specs=[block(shape[1]) for shape in shapes],
        ),
        input_output_aliases={2 + i: i for i in range(len(into))},
        compiler_params=pltpu.CompilerParams(vmem_limit_bytes=16 * 2**20),
        cost_estimate=pl.CostEstimate(flops=10**8, bytes_accessed=4 * 10**6, transcendentals=0),
    )(place, source, *into)


def other_place(x, axis):
    size = lax.axis_size(axis)
    return lax.ppermute(x, axis, [(i, i ^ 1) for i in range(size)])


def exchange(x, axes):
    return lax.all_to_all(x, axes, split_axis=0, concat_axis=0, tiled=True)


def swap(x, partner):
    return lax.ppermute(x, AXES, [(d, partner(d)) for d in range(lax.axis_size(AXES))])


def block_order():
    order = []
    for d in range(lax.axis_size(PLANE)):
        core, near, far = d & 1, (d >> 1) & 1, d >> 2
        first, second = (near, far) if core else (far, near)
        order.append((core * 2 + first) * 2 + second)
    return order


def weight_sum(early, keep, give):
    total, plane = lax.axis_size(AXES), lax.axis_size(PLANE)
    me = lax.axis_index(AXES)
    early = exchange(early.reshape(plane, early.shape[0] // plane, early.shape[1]), PLANE)
    early = jnp.sum(early.astype(F32), axis=0).astype(BF)

    by_core = lambda first, second: (lambda d: d ^ (1 << (second if d & 1 else first)))
    upper = lambda first, second: (me >> jnp.where(me & 1 == 1, second, first)) & 1
    bits = range(3, total.bit_length() - 1)

    def sum_line(x):
        for first, second in zip(bits, bits[::-1]):
            got = swap(x, by_core(first, second))
            x = (x.astype(F32) + got.astype(F32)).astype(BF)
        return x

    early = sum_line(early)
    got = other_place(give, "s0")
    x = (keep.astype(F32) + got.astype(F32)).astype(BF)
    for first, second in ((2, 1), (1, 2)):
        halves = x.reshape(2, x.shape[0] // 2, x.shape[1])
        place = upper(first, second)
        mine = lax.dynamic_index_in_dim(halves, place, 0, keepdims=False)
        give = lax.dynamic_index_in_dim(halves, 1 - place, 0, keepdims=False)
        got = swap(give, by_core(first, second))
        x = (mine.astype(F32) + got.astype(F32)).astype(BF)
    x = jnp.concatenate([early, sum_line(x)], axis=1)
    for first, second in ((1, 2), (2, 1)):
        got = swap(x, by_core(first, second))
        place = upper(first, second) == 1
        x = jnp.concatenate([jnp.where(place, got, x), jnp.where(place, x, got)], axis=0)
    return x, other_place(x, "s0")


def on_device(item_table, fetch_rows, event_slot, lengths, in_weight, out_weight, out_grad):
    emb = ("e1", "e0")
    shard_rows, width = item_table.shape
    requests = fetch_rows.reshape(lax.axis_size(emb), -1)
    slots = requests.shape[0] * requests.shape[1]
    tokens = event_slot.shape[0]
    asked = exchange(requests, emb)
    found = item_table[asked]
    fetched = exchange(found, emb)
    rows = fetched.reshape(slots, width)
    slot_row, slot_col = event_slot.reshape(1, tokens), event_slot.reshape(tokens, 1)
    core = lax.axis_index("s0").reshape(1, 1)
    count = len(GROUPS)

    dgated, res = call(
        early_kernel, [((tokens, width), BF), ((slots, width), F32)], [], [VMEM] * 3, 10**9
    )(slot_row, out_weight, out_grad)
    first = call_first(block_order(), tokens, slots, width)
    outs = first(lengths, slot_row, slot_col, rows, in_weight, out_weight, out_grad, dgated)
    layer_out, wg, nt, dpre_gate = outs[:4]
    vqk, datt, dsil = (outs[4 + k * count : 4 + (k + 1) * count] for k in range(3))

    slot_grad, keep, give = call_attention(tokens, slots, width)(
        lengths, core, slot_row, vqk[0], datt[0], dsil[0], nt, in_weight, rows, res, dpre_gate
    )
    own, got = weight_sum(wg, keep, give)
    returned = exchange(slot_grad.reshape(requests.shape + (width,)), emb)
    arrays, places = [returned.reshape(slots, width)], [asked.reshape(1, slots)]
    for axis in ("s1", "s0"):
        places += [other_place(p, axis) for p in places]
        arrays += [other_place(a, axis) for a in arrays]
    quarter = shard_rows // lax.axis_size(("s1", "s0"))
    base = lax.axis_index(("s1", "s0")) * quarter
    places = [p - base for p in places]
    (table_grad,) = call(
        functools.partial(table_kernel, len(places)),
        [((quarter, width), F32)],
        [],
        [VMEM] * (2 * len(places)),
        10**9,
        24,
    )(*places, *arrays)
    place = core.reshape(1)
    laid = lay(place, own, width)
    in_total, out_total = lay(1 - place, got, width, *laid)
    return layer_out, table_grad, in_total, out_total


def solution(mesh):
    emb, seq = mesh.shape["emb"], mesh.shape["seq"]
    fine = jax.sharding.Mesh(mesh.devices.reshape(emb // 2, 2, seq // 2, 2), AXES)
    placed = (
        P(("e1", "e0"), None),
        P(("e1", "e0"), ("s1", "s0"), None, None),
        P(AXES),
        P(AXES, None),
        P(),
        P(),
        P(AXES, None),
    )


    return jax.shard_map(
        on_device,
        mesh=fine,
        in_specs=placed,
        out_specs=(P(AXES, None), P(AXES, None), P(), P()),
        check_vma=False,
    )
```

```python
import functools

import jax
import jax.numpy as jnp
from jax import lax
from jax.experimental import pallas as pl
from jax.experimental.pallas import tpu as pltpu
from jax.sharding import PartitionSpec as P


HEADS = 4
MOST = 512
EPS = 1e-05
BLOCK = 256
MIB = 56
GROUPS = ((0, HEADS),)
VMEM = pl.BlockSpec(memory_space=pltpu.VMEM)
SMEM = pl.BlockSpec(memory_space=pltpu.SMEM)
ANY = pl.BlockSpec(memory_space=pl.ANY)
BF = jnp.bfloat16
F32 = jnp.float32


AXES = ("e1", "e0", "s1", "s0")
PLANE = AXES[1:]


def mm(a, b):
    return jnp.dot(a, b, preferred_element_type=F32)


def mm_t(a, b):
    return lax.dot_general(a, b, (((1,), (1,)), ((), ())), preferred_element_type=F32)


def tt_mm(a, b):
    return lax.dot_general(a, b, (((0,), (0,)), ((), ())), preferred_element_type=F32)


def center_rows(x):
    center = x - jnp.mean(x, axis=-1, keepdims=True)
    spread = jnp.mean(center * center, axis=-1, keepdims=True)
    inverse = lax.rsqrt(spread + EPS)
    return center * inverse, inverse


def center_back(grad, normed, inverse):
    along = jnp.mean(grad * normed, axis=-1, keepdims=True)
    return inverse * (grad - jnp.mean(grad, axis=-1, keepdims=True) - normed * along)


def history_ends(len_ref):
    ends, total = [], 0
    for k in range(len_ref.shape[1]):
        total = total + len_ref[0, k]
        ends.append(total)
    return ends


def history_start(ends, place):
    start = jnp.zeros_like(place)
    for end in ends:
        start = jnp.maximum(start, jnp.where(place >= end, end, 0))
    return start


def one_hot_rows(slot_row, slots):
    at = lax.broadcasted_iota(jnp.int32, (slots, slot_row.shape[1]), 0)
    return jnp.where(slot_row[...] == at, 1.0, 0.0).astype(BF)


def gather_kernel(asked_ref, table_ref, out_ref, total):
    step, rows = pl.program_id(0), table_ref.shape[0]
    lane = step * rows + lax.broadcasted_iota(jnp.int32, (asked_ref.shape[1], rows), 1)
    columns = asked_ref[...].T
    picks = [
        jnp.where(columns[:, o : o + 1] == lane, 1.0, 0.0).astype(BF) for o in range(asked_ref.shape[0])
    ]
    part = mm(jnp.concatenate(picks, axis=0), table_ref[...])

    @pl.when(step == 0)
    def _():
        total[...] = part

    @pl.when(step > 0)
    def _():
        total[...] += part

    @pl.when(step == pl.num_programs(0) - 1)
    def _():
        out_ref[...] = total[...].astype(BF)


def early_kernel(slot_row, wout_ref, og_ref, dgated_ref, res_ref):
    slots = res_ref.shape[0]
    dgated_ref[...] = mm_t(og_ref[...], wout_ref[...]).astype(BF)
    res_ref[...] = mm(one_hot_rows(slot_row, slots), og_ref[...])


def blocks(ref, order, cols, value):
    rows = value.shape[0] // len(order)
    for i, block in enumerate(order):
        ref[i * rows : (i + 1) * rows, cols] = value[block * rows : (block + 1) * rows, :]


def first_kernel(order, len_ref, slot_row, slot_col, rows_ref, *refs):
    sources, targets = refs[:4], refs[4:11]
    held, kept = refs[11:15], refs[15:22]
    hid, gate, ev, att, gated, dgate, dsil_gate, sems = refs[22:]
    loads = [pltpu.make_async_copy(sources[i], held[i], sems.at[i]) for i in range(4)]
    stores = [pltpu.make_async_copy(kept[i], targets[i], sems.at[4 + i]) for i in range(7)]
    win_ref, wout_ref, og_ref, dgated_ref = held
    out_ref, wg_ref, nt_ref, dpre_ref, vqk, datt, dsil = kept
    vqk, datt, dsil = (vqk,), (datt,), (dsil,)
    for load in loads:
        load.start()
    slots, width = rows_ref.shape
    tokens = og_ref.shape[0]
    head = width // HEADS
    half_scale = 0.5 * head**-0.5
    normed, _ = center_rows(rows_ref[...].astype(F32))
    normed = normed.astype(BF)
    nt_ref[...] = normed.T
    stores[2].start()
    loads[0].wait()
    for j in range(4):
        cols = slice(j * width, (j + 1) * width)
        pre = mm(normed, win_ref[:, cols])
        sig = 0.5 + 0.5 * jnp.tanh(0.5 * pre)
        act = pre * sig
        hid[:, cols] = act.astype(BF)
        slope = (sig + act * (1.0 - sig)).astype(BF)
        if j == 0:
            dsil_gate[...] = slope
        else:
            for (h0, h1), ref in zip(GROUPS, dsil):
                wide = (h1 - h0) * head
                ref[:, (j - 1) * wide : j * wide] = slope[:, h0 * head : h1 * head]

    stores[6].start()

    def spread(i, _):
        span = pl.ds(pl.multiple_of(i * BLOCK, BLOCK), BLOCK)
        lane = lax.broadcasted_iota(jnp.int32, (BLOCK, slots), 1)
        pick = jnp.where(slot_col[span, :] == lane, 1.0, 0.0).astype(BF)
        ev[span, :] = mm(pick, rows_ref[...]).astype(BF)
        gate[span, :] = mm(pick, hid[:, :width]).astype(BF)
        for j in range(3):
            part = mm(pick, hid[:, (j + 1) * width : (j + 2) * width]).astype(BF)
            for (h0, h1), ref in zip(GROUPS, vqk):
                wide = (h1 - h0) * head
                ref[span, j * wide : (j + 1) * wide] = part[:, h0 * head : h1 * head]
        return 0

    lax.fori_loop(0, tokens // BLOCK, spread, 0)
    stores[4].start()
    for load in loads[1:]:
        load.wait()
    ends = history_ends(len_ref)

    def rows_step(i, _):
        base = pl.multiple_of(i * BLOCK, BLOCK)
        span = pl.ds(base, BLOCK)
        start = history_start(ends, base + lax.broadcasted_iota(jnp.int32, (BLOCK, 1), 0))
        place = base + lax.broadcasted_iota(jnp.int32, (BLOCK, BLOCK), 0)
        att[...] = jnp.zeros_like(att)

        def keys_step(j, _):
            key_base = pl.multiple_of(j * BLOCK, BLOCK)
            keys = pl.ds(key_base, BLOCK)
            other = key_base + lax.broadcasted_iota(jnp.int32, (BLOCK, BLOCK), 1)
            allowed = (other >= start) & (other <= place)
            parts = []
            for (h0, h1), ref in zip(GROUPS, vqk):
                wide = (h1 - h0) * head
                for lo in range(0, wide, head):
                    q = ref[span, wide + lo : wide + lo + head]
                    k = ref[keys, 2 * wide + lo : 2 * wide + lo + head]
                    u = mm_t(q, k) * half_scale
                    w = jnp.where(allowed, u + u * jnp.tanh(u), 0.0).astype(BF)
                    parts.append(mm(w, ref[keys, lo : lo + head]))
            for h, part in enumerate(parts):
                att[:, h * head : (h + 1) * head] += part
            return 0

        lax.fori_loop(history_start(ends, base) // BLOCK, i + 1, keys_step, 0)
        normed_att, inverse = center_rows(att[...] * (1.0 / MOST))
        g = gate[span, :].astype(F32)
        gated_rows = (normed_att * g).astype(BF)
        gated[span, :] = gated_rows
        out_ref[span, :] = (mm(gated_rows, wout_ref[...]) + ev[span, :].astype(F32)).astype(BF)
        dgated = dgated_ref[span, :].astype(F32)
        dgate[span, :] = (dgated * normed_att).astype(BF)
        back = (center_back(dgated * g, normed_att, inverse) * (1.0 / MOST)).astype(BF)
        for (h0, h1), ref in zip(GROUPS, datt):
            ref[span, :] = back[:, h0 * head : h1 * head]
        return 0

    lax.fori_loop(0, tokens // BLOCK, rows_step, 0)
    stores[0].start()
    stores[5].start()
    blocks(wg_ref, order, slice(0, width), tt_mm(gated[...], og_ref[...]).astype(BF))
    slot_sum = mm(one_hot_rows(slot_row, slots), dgate[...])
    dpre = (slot_sum * dsil_gate[...].astype(F32)).astype(BF)
    dpre_ref[...] = dpre
    stores[3].start()
    blocks(wg_ref, order, slice(width, 2 * width), mm(nt_ref[...], dpre).astype(BF))
    stores[1].start()
    for store in stores:
        store.wait()


def second_kernel(len_ref, core_ref, slot_row, *refs):
    sources, targets = refs[:8], refs[8:11]
    vqk_ref, datt_ref, dsil_ref, nt_ref, win_ref, rows_ref, res_ref, gate_ref = refs[11:19]
    grad_ref, keep_ref, give_ref, dpre_ref, kt = refs[19:24]
    sums, sems = refs[24:-1], refs[-1]
    heads, tokens = HEADS, datt_ref.shape[0]
    slots, wide = dpre_ref.shape[0], datt_ref.shape[1]
    head = wide // heads
    half_scale = 0.5 * head**-0.5
    steps = tokens // BLOCK

    def loads(i):
        span = pl.ds(pl.multiple_of(i * BLOCK, BLOCK), BLOCK)
        return [
            pltpu.make_async_copy(source.at[span], ref.at[span], sems.at[k * steps + i])
            for k, (source, ref) in enumerate(((sources[0], vqk_ref), (sources[1], datt_ref)))
        ]

    late = [
        pltpu.make_async_copy(source, ref, sems.at[2 * steps + k])
        for k, (source, ref) in enumerate(zip(sources[2:], refs[13:19]))
    ]
    stores = [
        pltpu.make_async_copy(ref, target, sems.at[2 * steps + 6 + k])
        for k, (ref, target) in enumerate(zip((grad_ref, keep_ref, give_ref), targets))
    ]
    for i in range(steps):
        for load in loads(i):
            load.start()
    for load in late:
        load.start()
    ends = history_ends(len_ref)
    for ref in sums:
        ref[...] = jnp.zeros_like(ref)

    def rows_step(i, _):
        base = pl.multiple_of(i * BLOCK, BLOCK)
        span = pl.ds(base, BLOCK)
        for load in loads(i):
            load.wait()
        kt[:, span] = vqk_ref[span, 2 * wide :].T
        start = history_start(ends, base + lax.broadcasted_iota(jnp.int32, (1, BLOCK), 1))
        place = base + lax.broadcasted_iota(jnp.int32, (BLOCK, BLOCK), 1)

        def keys_step(j, _):
            key_base = pl.multiple_of(j * BLOCK, BLOCK)
            keys = pl.ds(key_base, BLOCK)
            other = key_base + lax.broadcasted_iota(jnp.int32, (BLOCK, BLOCK), 0)
            allowed = jnp.where((other >= start) & (other <= place), 1.0, 0.0).astype(BF)
            one, half = jnp.asarray(1.0, BF), jnp.asarray(half_scale, BF)
            parts = []
            for h in range(heads):
                lo = h * head
                q = vqk_ref[span, wide + lo : wide + lo + head]
                k = vqk_ref[keys, 2 * wide + lo : 2 * wide + lo + head]
                v = vqk_ref[keys, lo : lo + head]
                da = datt_ref[span, lo : lo + head]
                u = (mm_t(k, q) * half_scale).astype(BF)
                dw = mm_t(v, da).astype(BF) * allowed
                th = jnp.tanh(u)
                uth = u * th
                w = (u + uth) * allowed
                ds = dw * ((half + half * th) * (one + (u - uth)))
                parts.append((mm(w, da), mm(kt[lo : lo + head, keys], ds), mm(ds, q)))
            for h in range(heads):
                sums[3 * h][keys, :] += parts[h][0]
                sums[3 * h + 1][:, span] += parts[h][1]
                sums[3 * h + 2][keys, :] += parts[h][2]
            return 0

        lax.fori_loop(history_start(ends, base) // BLOCK, i + 1, keys_step, 0)
        return 0

    lax.fori_loop(0, steps, rows_step, 0)
    put = one_hot_rows(slot_row, slots)
    for load in late:
        load.wait()
    dn = mm_t(gate_ref[...], win_ref[:, :wide])
    for j in range(3):
        parts = [sums[3 * h + j][...].astype(BF) for h in range(heads)]
        cols = slice(j * wide, (j + 1) * wide)
        if j == 1:
            slot_sum = mm_t(put, jnp.concatenate(parts, axis=0))
        else:
            slot_sum = mm(put, jnp.concatenate(parts, axis=1))
        dpre = (slot_sum * dsil_ref[:, cols].astype(F32)).astype(BF)
        dpre_ref[:, cols] = dpre
        dn = dn + mm_t(dpre, win_ref[:, (j + 1) * wide : (j + 2) * wide])
    normed, inverse = center_rows(rows_ref[...].astype(F32))
    grad_ref[...] = (center_back(dn, normed, inverse) + res_ref[...]).astype(BF)
    stores[0].start()
    half = nt_ref.shape[0] // 2
    for k, ref, place in ((2, give_ref, 1 - core_ref[0, 0]), (1, keep_ref, core_ref[0, 0])):
        span = pl.ds(pl.multiple_of(place * half, half), half)
        ref[...] = mm(nt_ref[span, :], dpre_ref[...]).astype(BF)
        stores[k].start()
    for store in stores:
        store.wait()


def lay_kernel(place_ref, source, *refs):
    in_ref, out_ref = refs[-2:]
    width = out_ref.shape[1]
    out_ref[...] = source[:, :width].astype(F32)
    in_ref[...] = source[:, width:].astype(F32)


def table_kernel(count, *refs):
    places, rows, out = refs[:count], refs[count : 2 * count], refs[-1]
    height = min(BLOCK, out.shape[0])

    def step(i, _):
        base = pl.multiple_of(i * height, height)
        total = None
        for place, row in zip(places, rows):
            at = base + lax.broadcasted_iota(jnp.int32, (height, place.shape[1]), 0)
            put = jnp.where(place[...] == at, 1.0, 0.0).astype(BF)
            part = mm(put, row[...])
            total = part if total is None else total + part
        out[pl.ds(base, height), :] = total
        return 0

    lax.fori_loop(0, out.shape[0] // height, step, 0)


def call(kernel, outs, scratch, specs, flops, mib=MIB, own_copies=0):
    semaphores = [pltpu.SemaphoreType.DMA((own_copies,))] if own_copies else []
    return pl.pallas_call(
        kernel,
        out_shape=[jax.ShapeDtypeStruct(s, d) for s, d in outs],
        in_specs=specs,
        out_specs=[ANY if own_copies else VMEM] * len(outs),
        scratch_shapes=[pltpu.VMEM(s, d) for s, d in scratch] + semaphores,
        compiler_params=pltpu.CompilerParams(vmem_limit_bytes=mib * 2**20),
        cost_estimate=pl.CostEstimate(flops=flops, bytes_accessed=10**7, transcendentals=0),
    )


def gather(table, asked, steps=2):
    slots, rows, width = asked.shape[0] * asked.shape[1], table.shape[0] // steps, table.shape[1]
    return pl.pallas_call(
        gather_kernel,
        out_shape=jax.ShapeDtypeStruct((slots, width), BF),
        grid=(steps,),
        in_specs=[pl.BlockSpec(asked.shape, lambda i: (0, 0)), pl.BlockSpec((rows, width), lambda i: (i, 0))],
        out_specs=pl.BlockSpec((slots, width), lambda i: (0, 0)),
        scratch_shapes=[pltpu.VMEM((slots, width), F32)],
        compiler_params=pltpu.CompilerParams(vmem_limit_bytes=MIB * 2**20),
        cost_estimate=pl.CostEstimate(flops=10**9, bytes_accessed=10**7, transcendentals=0),
    )(asked, table)


def call_first(order, tokens, slots, width):
    loads = [((width, 4 * width), BF), ((width, width), BF), ((tokens, width), BF), ((tokens, width), BF)]
    outs = [
        ((tokens, width), BF), ((width, 2 * width), BF), ((width, slots), BF), ((slots, width), BF),
        ((tokens, 3 * width), BF), ((tokens, width), BF), ((slots, 3 * width), BF),
    ]
    return call(
        functools.partial(first_kernel, order),
        outs,
        loads + outs
        + [
            ((slots, 4 * width), BF), ((tokens, width), BF), ((tokens, width), BF), ((BLOCK, width), F32),
            ((tokens, width), BF), ((tokens, width), BF), ((slots, width), BF),
        ],
        [SMEM] + [VMEM] * 3 + [ANY] * 4,
        10**10,
        own_copies=len(loads) + len(outs),
    )


def call_attention(tokens, slots, width):
    head, grads = width // HEADS, 3 * width
    loads = [
        ((tokens, grads), BF), ((tokens, width), BF), ((slots, grads), BF), ((width, slots), BF),
        ((width, 4 * width), BF), ((slots, width), BF), ((slots, width), F32), ((slots, width), BF),
    ]
    outs = [((slots, width), BF)] + [((width // 2, grads), BF)] * 2
    sums = [((tokens, head), F32), ((head, tokens), F32), ((tokens, head), F32)] * HEADS
    return call(
        second_kernel,
        outs,
        loads + outs + [((slots, grads), BF), ((width, tokens), BF)] + sums,
        [SMEM] * 2 + [VMEM] + [ANY] * 8,
        10**10,
        own_copies=2 * (tokens // BLOCK) + 9,
    )


def lay(place, source, width, *into):
    half, steps = source.shape[0], 4
    rows = half // steps
    block = lambda columns: pl.BlockSpec((rows, columns), lambda i, place_ref: (place_ref[0] * steps + i, 0))
    shapes = [(2 * half, source.shape[1] - width), (2 * half, width)]
    return pl.pallas_call(
        lay_kernel,
        out_shape=[jax.ShapeDtypeStruct(s, F32) for s in shapes],
        grid_spec=pltpu.PrefetchScalarGridSpec(
            num_scalar_prefetch=1,
            grid=(steps,),
            in_specs=[pl.BlockSpec((rows, source.shape[1]), lambda i, place_ref: (i, 0))]
            + [pl.BlockSpec(memory_space=pl.ANY)] * len(into),
            out_specs=[block(shape[1]) for shape in shapes],
        ),
        input_output_aliases={2 + i: i for i in range(len(into))},
        compiler_params=pltpu.CompilerParams(vmem_limit_bytes=16 * 2**20),
        cost_estimate=pl.CostEstimate(flops=10**8, bytes_accessed=4 * 10**6, transcendentals=0),
    )(place, source, *into)


def other_place(x, axis):
    size = lax.axis_size(axis)
    return lax.ppermute(x, axis, [(i, i ^ 1) for i in range(size)])


def exchange(x, axes):
    return lax.all_to_all(x, axes, split_axis=0, concat_axis=0, tiled=True)


def swap(x, partner):
    return lax.ppermute(x, AXES, [(d, partner(d)) for d in range(lax.axis_size(AXES))])


def block_order():
    order = []
    for d in range(lax.axis_size(PLANE)):
        core, near, far = d & 1, (d >> 1) & 1, d >> 2
        first, second = (near, far) if core else (far, near)
        order.append((core * 2 + first) * 2 + second)
    return order


def weight_sum(early, keep, give):
    total, plane = lax.axis_size(AXES), lax.axis_size(PLANE)
    me = lax.axis_index(AXES)
    early = exchange(early.reshape(plane, early.shape[0] // plane, early.shape[1]), PLANE)
    early = jnp.sum(early.astype(F32), axis=0).astype(BF)

    by_core = lambda first, second: (lambda d: d ^ (1 << (second if d & 1 else first)))
    upper = lambda first, second: (me >> jnp.where(me & 1 == 1, second, first)) & 1
    bits = range(3, total.bit_length() - 1)

    def sum_line(x):
        for first, second in zip(bits, bits[::-1]):
            got = swap(x, by_core(first, second))
            x = (x.astype(F32) + got.astype(F32)).astype(BF)
        return x

    early = sum_line(early)
    got = other_place(give, "s0")
    x = (keep.astype(F32) + got.astype(F32)).astype(BF)
    for first, second in ((2, 1), (1, 2)):
        halves = x.reshape(2, x.shape[0] // 2, x.shape[1])
        place = upper(first, second)
        mine = lax.dynamic_index_in_dim(halves, place, 0, keepdims=False)
        give = lax.dynamic_index_in_dim(halves, 1 - place, 0, keepdims=False)
        got = swap(give, by_core(first, second))
        x = (mine.astype(F32) + got.astype(F32)).astype(BF)
    x = jnp.concatenate([early, sum_line(x)], axis=1)
    for first, second in ((1, 2), (2, 1)):
        got = swap(x, by_core(first, second))
        place = upper(first, second) == 1
        x = jnp.concatenate([jnp.where(place, got, x), jnp.where(place, x, got)], axis=0)
    return x, other_place(x, "s0")


def on_device(item_table, fetch_rows, event_slot, lengths, in_weight, out_weight, out_grad):
    emb = ("e1", "e0")
    shard_rows, width = item_table.shape
    requests = fetch_rows.reshape(lax.axis_size(emb), -1)
    slots = requests.shape[0] * requests.shape[1]
    tokens = event_slot.shape[0]
    asked = exchange(requests, emb)
    found = gather(item_table, asked).reshape(asked.shape + (width,))
    fetched = exchange(found, emb)
    rows = fetched.reshape(slots, width)
    slot_row, slot_col = event_slot.reshape(1, tokens), event_slot.reshape(tokens, 1)
    core = lax.axis_index("s0").reshape(1, 1)
    count = len(GROUPS)

    dgated, res = call(
        early_kernel, [((tokens, width), BF), ((slots, width), F32)], [], [VMEM] * 3, 10**9
    )(slot_row, out_weight, out_grad)
    first = call_first(block_order(), tokens, slots, width)
    outs = first(lengths, slot_row, slot_col, rows, in_weight, out_weight, out_grad, dgated)
    layer_out, wg, nt, dpre_gate = outs[:4]
    vqk, datt, dsil = (outs[4 + k * count : 4 + (k + 1) * count] for k in range(3))

    slot_grad, keep, give = call_attention(tokens, slots, width)(
        lengths, core, slot_row, vqk[0], datt[0], dsil[0], nt, in_weight, rows, res, dpre_gate
    )
    own, got = weight_sum(wg, keep, give)
    returned = exchange(slot_grad.reshape(requests.shape + (width,)), emb)
    arrays, places = [returned.reshape(slots, width)], [asked.reshape(1, slots)]
    for axis in ("s1", "s0"):
        places += [other_place(p, axis) for p in places]
        arrays += [other_place(a, axis) for a in arrays]
    quarter = shard_rows // lax.axis_size(("s1", "s0"))
    base = lax.axis_index(("s1", "s0")) * quarter
    places = [p - base for p in places]
    (table_grad,) = call(
        functools.partial(table_kernel, len(places)),
        [((quarter, width), F32)],
        [],
        [VMEM] * (2 * len(places)),
        10**9,
        24,
    )(*places, *arrays)
    place = core.reshape(1)
    laid = lay(place, own, width)
    in_total, out_total = lay(1 - place, got, width, *laid)
    return layer_out, table_grad, in_total, out_total


def solution(mesh):
    emb, seq = mesh.shape["emb"], mesh.shape["seq"]
    fine = jax.sharding.Mesh(mesh.devices.reshape(emb // 2, 2, seq // 2, 2), AXES)
    placed = (
        P(("e1", "e0"), None),
        P(("e1", "e0"), ("s1", "s0"), None, None),
        P(AXES),
        P(AXES, None),
        P(),
        P(),
        P(AXES, None),
    )


    return jax.shard_map(
        on_device,
        mesh=fine,
        in_specs=placed,
        out_specs=(P(AXES, None), P(AXES, None), P(), P()),
        check_vma=False,
    )
```
